32 devices in a mesh: parts: 2 (over x), dp: 16 (over z, y, core).
Axes of the slice: x: 2, y: 2, z: 4, core: 2. Of those that a mesh axis runs over, the one named last changes fastest.
Arguments:
- activations: bfloat16 [8192, 14336], P(('parts', 'dp')), parts along dimension 0, may hold values from -6 to 6
- out_grads: bfloat16 [8192, 4096], P(('parts', 'dp')), parts along dimension 0, may hold values from -6 to 6
- lengths: int32 [32, 4], P(('parts', 'dp')), parts along dimension 0, may hold values from 1 to 128, 256 in all within a row
- proj_in: bfloat16 [14336, 64], replicated, may hold values from -0.046875 to 0.046875
- proj_out: bfloat16 [4096, 64], replicated, may hold values from -0.09375 to 0.09375
- queries: bfloat16 [1024, 4096], P(('parts', 'dp')), parts along dimension 0, may hold values from -0.01171875 to 0.01171875
Outputs:
- scores: bfloat16 [128, 512], P(('parts', 'dp')), parts along dimension 0
The draws below stay inside these ranges and needn't reach their ends.
There are 2 independent parts, one for each index of `parts`. The reference program is written for one: setup_inputs(seed, part) draws one part's arguments, and reference() takes and returns one part's arrays. A program takes and returns all parts, laid end to end along the dimension named above; an argument that names none is the same for every part. Nothing has to cross between parts.
Inputs may be any that keep to these rules, and one draw needn't show every extreme that they name: Each row of lengths sums to 256, and one entry of each row equals 128.
All inputs are finite; a program needn't handle non-finite values.
Results may differ from the reference program's by a relative error of at most 0.0065.
Values may be sent and summed in bfloat16 or wider, within the bound.
A program may use at most 128 MiB of HBM per device.

```python
import math
import jax
import jax.numpy as jnp
import numpy as np

D = 4096
FF = 14336
RANK = 64
TOK_DEV = 256
EX_DEV = 4
TOKENS = 4096
N_TRAIN = 64
NQ = 512
PARAMS = 4096
MOST = 128
N_DP = 16


def level_of(rng, dims, pieces, smallest, top_value):
    level = 1.0
    for dim, shards_of in pieces:
        heights = jax.random.uniform(jax.random.fold_in(jax.random.fold_in(rng, 6), dim), (shards_of,), jnp.float32, smallest / len(pieces), top_value / len(pieces))
        level = level * jnp.repeat(jnp.exp(heights), dims[dim] // shards_of).reshape((-1,) + (1,) * (len(dims) - 1 - dim))
    return level


def split_up(number_of, total, reach, lean):
    weights = [(1 << 20) // math.isqrt(standing ** lean) + 1 for standing in range(2, number_of + 1)]
    surplus, holding = total - reach - (number_of - 1), [1] * (number_of - 1)
    while surplus > 0:
        free = [i for i in range(number_of - 1) if holding[i] < reach]
        mass, remaining = sum([weights[i] for i in free]), surplus
        for i in free:
            more = min(reach - holding[i], max(1, remaining * weights[i] // mass), surplus)
            holding[i] = holding[i] + more
            surplus = surplus - more
    return np.array([reach] + holding)


def uneven(own_key, count, total, reach, lean):
    if count == 2:
        one = jax.random.randint(own_key, (), max(1, total - reach), min(reach, total - 1) + 1)
        return jnp.stack([one, total - one])
    sizes = jnp.asarray(split_up(count, total, reach, lean), jnp.int32)
    twos = (count - 1) // 2
    giver, sink = sizes[1:1 + 2 * twos:2], sizes[2:2 + 2 * twos:2]
    room = jnp.minimum(giver - 1, reach - sink)
    shifted = jax.random.randint(jax.random.fold_in(own_key, 1), (twos,), 0, 1 << 20) % (room + 1)
    sizes = sizes.at[1:1 + 2 * twos:2].set(giver - shifted).at[2:2 + 2 * twos:2].set(sink + shifted)
    return sizes[jax.random.permutation(jax.random.fold_in(own_key, 2), count)]


def scatter_about(own_key, extent, spread, reach, pieces=(), kind=jnp.bfloat16):
    entries = spread * jax.random.normal(own_key, extent, jnp.float32)
    if pieces:
        entries = entries * level_of(own_key, extent, pieces, -0.22, 0.18)
    return jnp.clip(entries, -reach, reach).astype(kind)


def setup_inputs(seed: int = 0, part: int = 0) -> dict:
    key_of = jax.random.split(jax.random.key(seed), 7)
    part_keys = jax.random.split(jax.random.fold_in(key_of[6], part), 7)
    activations = scatter_about(part_keys[0], (TOKENS, FF), 1.0, 6.0, ((0, 16),))
    out_grads = scatter_about(part_keys[1], (TOKENS, D), 1.0, 6.0, ((0, 16),))
    lengths = jax.vmap(lambda own: uneven(own, EX_DEV, TOK_DEV, MOST, 2))(jax.random.split(part_keys[2], N_DP)).reshape((N_DP, EX_DEV)).astype(jnp.int32)
    proj_in = scatter_about(key_of[3], (FF, RANK), FF ** -0.5, 0.046875)
    proj_out = scatter_about(key_of[4], (D, RANK), D ** -0.5, 0.09375)
    queries = scatter_about(part_keys[5], (NQ, PARAMS), (0.125 / RANK), 0.01171875, ((0, 16),))
    return dict(activations=activations, out_grads=out_grads, lengths=lengths, proj_in=proj_in, proj_out=proj_out, queries=queries)


def reference(activations, out_grads, lengths, proj_in, proj_out, queries):
    proj_acts = jnp.dot(activations, proj_in, preferred_element_type=jnp.float32).astype(jnp.bfloat16)
    proj_grads = jnp.dot(out_grads, proj_out, preferred_element_type=jnp.float32).astype(jnp.bfloat16)
    acts_wide = proj_acts.astype(jnp.float32)
    grads_wide = proj_grads.astype(jnp.float32)
    outer_terms = (grads_wide[:, :, None] * acts_wide[:, None, :]).reshape(TOKENS, RANK * RANK)
    tok_ends = jnp.cumsum(lengths.reshape(-1)).astype(jnp.int32)
    position = jnp.arange(TOKENS, dtype=jnp.int32)
    example_ids = jnp.searchsorted(tok_ends, position, side="right").astype(jnp.int32)
    example_grads = jax.ops.segment_sum(outer_terms, example_ids, num_segments=N_TRAIN).astype(jnp.bfloat16)
    return jnp.dot(example_grads, queries.T, preferred_element_type=jnp.float32).astype(jnp.bfloat16)
```

```python
import functools

import jax
import jax.numpy as jnp
from jax import lax
from jax.experimental import pallas as pl
from jax.experimental.pallas import tpu as pltpu
from jax.sharding import PartitionSpec as P

MESH = pl.DeviceIdType.MESH
NT = (((1,), (1,)), ((), ()))
NN = (((1,), (0,)), ((), ()))
PIECES = 8
EARLY = 1
AHEAD = 4
GROUP = 4
LANES = 128
ROWS = 16


def kernel(
    n,
    lens_hbm,
    acts_hbm,
    grads_hbm,
    win_hbm,
    wout_hbm,
    q_hbm,
    out,
    lens,
    acts,
    grads,
    win,
    wout,
    qs,
    eg,
    stage,
    local_sem,
    piece_sem,
    send_sem,
    buddy_recv,
    across_recv,
    relay_recv,
    eg_recv,
    res_recv,
):
    me = lax.axis_index("dp")
    n_groups = n // GROUP
    group, lane = me // GROUP, lax.rem(me, GROUP)
    tokens, ff = acts.shape
    rank = win.shape[0]
    ex = stage.shape[1]
    slots = ROWS // ex
    nq, params = qs.shape[1:]
    span = params // slots
    tiles = span // LANES
    half = tiles * ROWS
    cols = GROUP * nq
    piece = ff // PIECES

    backward = (group < n_groups - group).astype(jnp.int32)

    def project(rows, weights, at, size):
        parts = []
        for h in range(2):
            first = at + h * (size // 2 // LANES * LANES)
            last = at + (size // 2 // LANES * LANES if h == 0 else size)
            one = weights[:, first:last]
            twice = jnp.concatenate([one, one], axis=0)
            parts.append(
                lax.dot_general(rows[:, first:last], twice, NT, preferred_element_type=jnp.float32)
            )
        return parts[0] + parts[1]

    def turn(t):
        return t + backward * (n_groups - 2 * t)

    def peer(t):
        return lax.rem(group + turn(t), n_groups) * GROUP + lane

    buddy = me + 1 - 2 * lax.rem(me, 2)
    across = me + 2 - 4 * lax.rem(me // 2, 2)
    across_lane = lax.rem(across, GROUP)

    def start(source, target, sem):
        load = pltpu.make_async_copy(source, target, sem)
        load.start()
        return load

    load_q = start(q_hbm, qs.at[lane], local_sem.at[0])
    load_lens = start(lens_hbm, lens, local_sem.at[1])
    load_wout = start(wout_hbm, wout, local_sem.at[2])
    load_grads = start(grads_hbm, grads, local_sem.at[2])
    pieces = [pl.ds(p * piece, piece) for p in range(PIECES)]
    loads = {}

    def fetch(p):
        if p < PIECES:
            loads[p] = (
                start(win_hbm.at[:, pieces[p]], win.at[:, pieces[p]], piece_sem.at[p]),
                start(acts_hbm.at[:, pieces[p]], acts.at[:, pieces[p]], piece_sem.at[p]),
            )

    for p in range(EARLY):
        fetch(p)

    barrier = pltpu.get_barrier_semaphore()
    peers = [peer(t) for t in range(1, n_groups)]
    for other in peers + [buddy, across]:
        pl.semaphore_signal(barrier, inc=1, device_id={"dp": other}, device_id_type=MESH)

    def send(source, target, recv_sem, other):
        copy = pltpu.make_async_remote_copy(
            src_ref=source,
            dst_ref=target,
            send_sem=send_sem,
            recv_sem=recv_sem,
            device_id={"dp": other},
            device_id_type=MESH,
        )
        copy.start()
        return copy

    load_q.wait()
    for p in range(EARLY, AHEAD):
        fetch(p)
    pl.semaphore_wait(barrier, len(peers) + 2)
    sent = []
    across_copies = []
    for s in range(slots):
        part = qs.at[lane, :, pl.ds(s * span, span)]
        across_copies.append(send(part, part, across_recv.at[s], across))
    buddy_copy = send(qs.at[lane], qs.at[lane], buddy_recv, buddy)
    sent += across_copies + [buddy_copy]

    load_lens.wait()
    token = lax.broadcasted_iota(jnp.int32, (8, tokens), 1)
    row_ex = lax.rem(lax.broadcasted_iota(jnp.int32, (8, tokens), 0), ex)
    first = jnp.int32(0)
    mask = jnp.zeros((8, tokens), jnp.float32)
    for e in range(ex):
        end = first + lens[0, e]
        mask = jnp.where((row_ex == e) & (token >= first) & (token < end), 1.0, mask)
        first = end

    r_id = lax.broadcasted_iota(jnp.int32, (2 * half, 2 * rank), 0)
    c_id = lax.broadcasted_iota(jnp.int32, (2 * half, 2 * rank), 1)
    odd = (r_id >= half).astype(jnp.int32)
    inner = r_id - odd * half
    source = 2 * (lax.rem(inner // ex, slots) * tiles + inner // ROWS) + odd
    expand = jnp.where(source == c_id, 1.0, 0.0).astype(jnp.bfloat16)

    load_wout.wait()
    load_grads.wait()
    proj_grads = project(grads, wout, 0, wout.shape[1]).astype(jnp.bfloat16)
    wide = lax.dot_general(expand, proj_grads, NT, preferred_element_type=jnp.float32)
    wide = wide.reshape(2 * half // 8, 8, tokens) * mask[None]
    wide = wide.reshape(2 * half, tokens).astype(jnp.bfloat16)

    total = jnp.zeros((tokens, 2 * rank), jnp.float32)
    for p in range(PIECES):
        for load in loads[p]:
            load.wait()
        fetch(p + AHEAD)
        total = total + project(acts, win, p * piece, piece)
    proj_acts = total.astype(jnp.bfloat16)
    outer = lax.dot_general(wide, proj_acts, NN, preferred_element_type=jnp.float32)
    lower = lax.broadcasted_iota(jnp.int32, (half, 2 * rank), 1) < rank
    eg[group] = jnp.where(lower, outer[:half], outer[half:]).astype(jnp.bfloat16)

    eg_copies = []
    for t in range(1, n_groups):
        eg_copies.append(send(eg.at[group], eg.at[group], eg_recv, peer(t)))

    relays = []
    for s in range(slots):
        across_copies[s].wait_recv()
        part = qs.at[across_lane, :, pl.ds(s * span, span)]
        relays.append(send(part, part, relay_recv.at[s], buddy))
    buddy_copy.wait_recv()
    others = pl.ds(0, n_groups - 1)
    pltpu.make_async_copy(eg.at[others], eg.at[others], eg_recv).wait()

    stacked = []
    for g in range(n_groups):
        one = eg[g]
        stacked.append(
            jnp.concatenate([one[ROWS * t : ROWS * (t + 1)] for t in range(tiles)], axis=1)
        )
    stacked = jnp.concatenate(stacked, axis=0)
    scores = [jnp.zeros((ex, cols), jnp.float32) for _ in range(n_groups)]
    for s in range(slots):
        relays[s].wait_recv()
        queries = qs[:, :, pl.ds(s * span, span)].reshape(cols, span)
        term = 0.0
        for h in range(2):
            side = slice(h * (span // 2), (h + 1) * (span // 2))
            term = term + lax.dot_general(
                stacked[:, side], queries[:, side], NT, preferred_element_type=jnp.float32
            )
        for g in range(n_groups):
            row = ROWS * g + ex * s
            scores[g] = scores[g] + term[row : row + ex]
    for g in range(n_groups):
        stage[g] = scores[g].astype(jnp.bfloat16)

    own = pl.ds(pl.multiple_of(group * cols, LANES), cols)
    res_copies = []
    for t in range(1, n_groups):
        target = lax.rem(group + turn(t), n_groups)
        res_copies.append(
            send(stage.at[target], out.at[:, own], res_recv, peer(t))
        )
    out[:, own] = stage[group]
    rest = out.at[:, pl.ds(0, (n_groups - 1) * cols)]
    pltpu.make_async_copy(rest, rest, res_recv).wait()
    for copy in sent + eg_copies + relays + res_copies:
        copy.wait_send()


def local(n, activations, out_grads, lengths, proj_in, proj_out, queries):
    tokens, ff = activations.shape
    d = out_grads.shape[1]
    rank = proj_in.shape[1]
    ex = lengths.shape[1]
    nq, params = queries.shape
    n_groups = n // GROUP
    slots = ROWS // ex
    bf16 = jnp.bfloat16
    dma = pltpu.SemaphoreType.DMA
    hbm = pl.BlockSpec(memory_space=pltpu.MemorySpace.HBM)
    return pl.pallas_call(
        functools.partial(kernel, n),
        out_shape=jax.ShapeDtypeStruct((ex, nq * n), bf16),
        in_specs=[hbm] * 6,
        out_specs=pl.BlockSpec(memory_space=pltpu.MemorySpace.VMEM),
        scratch_shapes=[
            pltpu.SMEM((1, ex), jnp.int32),
            pltpu.VMEM((tokens, ff), bf16),
            pltpu.VMEM((tokens, d), bf16),
            pltpu.VMEM((rank, ff), bf16),
            pltpu.VMEM((rank, d), bf16),
            pltpu.VMEM((GROUP, nq, params), bf16),
            pltpu.VMEM((n_groups, ex * params // LANES, LANES), bf16),
            pltpu.VMEM((n_groups, ex, GROUP * nq), bf16),
            dma((3,)),
            dma((PIECES,)),
            dma,
            dma,
            dma((slots,)),
            dma((slots,)),
            dma,
            dma,
        ],
        compiler_params=pltpu.CompilerParams(
            collective_id=0, has_side_effects=True, vmem_limit_bytes=56500000
        ),
    )(pltpu.with_memory_space_constraint(lengths, pltpu.HBM), activations, out_grads, proj_in.T, proj_out.T, queries)


def solution(mesh):
    in_specs = (
        P(("parts", "dp"), None),
        P(("parts", "dp"), None),
        P(("parts", "dp"), None),
        P(),
        P(),
        P(("parts", "dp"), None),
    )
    out_specs = P(("parts", "dp"), None)
    body = functools.partial(local, mesh.shape["dp"])
    return jax.shard_map(body, mesh=mesh, in_specs=in_specs, out_specs=out_specs, check_vma=False)
```

```python
import functools

import jax
import jax.numpy as jnp
from jax import lax
from jax.experimental import pallas as pl
from jax.experimental.pallas import tpu as pltpu
from jax.sharding import PartitionSpec as P

MESH = pl.DeviceIdType.MESH
NT = (((1,), (1,)), ((), ()))
NN = (((1,), (0,)), ((), ()))
SHARES = (4, 4, 4, 4, 4, 4, 2, 2)
PIECES = len(SHARES)
EARLY = 1
AHEAD = 4
GROUP = 4
LANES = 128
ROWS = 16


def kernel(
    n,
    lens_hbm,
    acts_hbm,
    grads_hbm,
    win_hbm,
    wout_hbm,
    q_hbm,
    out,
    lens,
    acts,
    grads,
    win,
    wout,
    qs,
    eg,
    stage,
    wide,
    local_sem,
    piece_sem,
    send_sem,
    buddy_recv,
    across_recv,
    relay_recv,
    eg_recv,
    res_recv,
):
    me = lax.axis_index("dp")
    n_groups = n // GROUP
    group, lane = me // GROUP, lax.rem(me, GROUP)
    tokens, ff = acts.shape
    rank = win.shape[0]
    ex = stage.shape[1]
    slots = ROWS // ex
    nq, params = qs.shape[1:]
    span = params // slots
    tiles = span // LANES
    half = tiles * ROWS
    cols = GROUP * nq
    bounds = [ff * sum(SHARES[:p]) // sum(SHARES) for p in range(PIECES + 1)]

    backward = (group < n_groups - group).astype(jnp.int32)

    def project(sums, rows, weights, first, last):
        for h in range(2):
            side = slice(h * tokens // 2, (h + 1) * tokens // 2)
            part = lax.dot_general(
                weights[:, first:last],
                rows[side, first:last],
                NT,
                preferred_element_type=jnp.float32,
            )
            sums[h] = part if sums[h] is None else sums[h] + part

    def turn(t):
        return t + backward * (n_groups - 2 * t)

    def peer(t):
        return lax.rem(group + turn(t), n_groups) * GROUP + lane

    buddy = me + 1 - 2 * lax.rem(me, 2)
    across = me + 2 - 4 * lax.rem(me // 2, 2)
    across_lane = lax.rem(across, GROUP)

    def start(source, target, sem):
        load = pltpu.make_async_copy(source, target, sem)
        load.start()
        return load

    load_q = start(q_hbm, qs.at[lane], local_sem.at[0])
    load_lens = start(lens_hbm, lens, local_sem.at[1])
    load_wout = start(wout_hbm, wout, local_sem.at[2])
    load_grads = start(grads_hbm, grads, local_sem.at[2])
    pieces = [pl.ds(bounds[p], bounds[p + 1] - bounds[p]) for p in range(PIECES)]
    loads = {}

    def fetch(p):
        if p < PIECES:
            loads[p] = (
                start(win_hbm.at[:, pieces[p]], win.at[:, pieces[p]], piece_sem.at[p]),
                start(acts_hbm.at[:, pieces[p]], acts.at[:, pieces[p]], piece_sem.at[p]),
            )

    for p in range(EARLY):
        fetch(p)

    barrier = pltpu.get_barrier_semaphore()
    peers = [peer(t) for t in range(1, n_groups)]
    for other in peers + [buddy, across]:
        pl.semaphore_signal(barrier, inc=1, device_id={"dp": other}, device_id_type=MESH)

    def send(source, target, recv_sem, other):
        copy = pltpu.make_async_remote_copy(
            src_ref=source,
            dst_ref=target,
            send_sem=send_sem,
            recv_sem=recv_sem,
            device_id={"dp": other},
            device_id_type=MESH,
        )
        copy.start()
        return copy

    load_q.wait()
    for p in range(EARLY, AHEAD):
        fetch(p)
    pl.semaphore_wait(barrier, len(peers) + 2)
    sent = []
    across_copies = []
    for s in range(slots):
        part = qs.at[lane, :, pl.ds(s * span, span)]
        across_copies.append(send(part, part, across_recv.at[s], across))
    buddy_copy = send(qs.at[lane], qs.at[lane], buddy_recv, buddy)
    sent += across_copies + [buddy_copy]

    load_lens.wait()
    token = lax.broadcasted_iota(jnp.int32, (8, tokens), 1)
    row_ex = lax.rem(lax.broadcasted_iota(jnp.int32, (8, tokens), 0), ex)
    first = jnp.int32(0)
    mask = jnp.zeros((8, tokens), jnp.float32)
    for e in range(ex):
        end = first + lens[0, e]
        mask = jnp.where((row_ex == e) & (token >= first) & (token < end), 1.0, mask)
        first = end

    r_id = lax.broadcasted_iota(jnp.int32, (2 * half, rank), 0)
    c_id = lax.broadcasted_iota(jnp.int32, (2 * half, rank), 1)
    second = (r_id >= half).astype(jnp.int32)
    inner = r_id - second * half
    source = 2 * (lax.rem(inner // ex, slots) * tiles + inner // ROWS) + second
    expand = jnp.where(source == c_id, 1.0, 0.0).astype(jnp.bfloat16)

    load_wout.wait()
    load_grads.wait()
    sums = [None, None]
    project(sums, grads, wout, 0, wout.shape[1])
    proj_grads = jnp.concatenate(sums, axis=1).astype(jnp.bfloat16)

    sums = [None, None]
    for p in range(PIECES):
        for load in loads[p]:
            load.wait()
        fetch(p + AHEAD)
        project(sums, acts, win, bounds[p], bounds[p + 1])
        if p == 0:
            for h in range(2):
                side = slice(h * half, (h + 1) * half)
                part = lax.dot_general(
                    expand[side], proj_grads, NN, preferred_element_type=jnp.float32
                )
                part = part.reshape(half // 8, 8, tokens) * mask[None]
                wide[side] = part.reshape(half, tokens).astype(jnp.bfloat16)
    proj_acts = jnp.concatenate(sums, axis=1).astype(jnp.bfloat16)
    twice = jnp.concatenate([proj_acts, proj_acts], axis=0)
    even = lax.dot_general(wide[:half], twice, NT, preferred_element_type=jnp.float32)
    odd = lax.dot_general(wide[half:], twice, NT, preferred_element_type=jnp.float32)
    lower = lax.broadcasted_iota(jnp.int32, (half, 2 * rank), 1) < rank
    eg[group] = jnp.where(lower, even, odd).astype(jnp.bfloat16)

    eg_copies = []
    for t in range(1, n_groups):
        eg_copies.append(send(eg.at[group], eg.at[group], eg_recv, peer(t)))

    relays = []
    for s in range(slots):
        across_copies[s].wait_recv()
        part = qs.at[across_lane, :, pl.ds(s * span, span)]
        relays.append(send(part, part, relay_recv.at[s], buddy))
    buddy_copy.wait_recv()
    others = pl.ds(0, n_groups - 1)
    pltpu.make_async_copy(eg.at[others], eg.at[others], eg_recv).wait()

    stacked = []
    for g in range(n_groups):
        one = eg[g]
        stacked.append(
            jnp.concatenate([one[ROWS * t : ROWS * (t + 1)] for t in range(tiles)], axis=1)
        )
    stacked = jnp.concatenate(stacked, axis=0)
    scores = [None] * n_groups
    for early in (range(slots - 1), range(slots - 1, slots)):
        for s in early:
            relays[s].wait_recv()
        for s in early:
            queries = qs[:, :, pl.ds(s * span, span)].reshape(cols, span)
            term = lax.dot_general(stacked, queries, NT, preferred_element_type=jnp.float32)
            for g in range(n_groups):
                row = ROWS * g + ex * s
                part = term[row : row + ex]
                scores[g] = part if scores[g] is None else scores[g] + part
    for g in range(n_groups):
        stage[g] = scores[g].astype(jnp.bfloat16)

    own = pl.ds(pl.multiple_of(group * cols, LANES), cols)
    res_copies = []
    for t in range(1, n_groups):
        target = lax.rem(group + turn(t), n_groups)
        res_copies.append(
            send(stage.at[target], out.at[:, own], res_recv, peer(t))
        )
    out[:, own] = stage[group]
    rest = out.at[:, pl.ds(0, (n_groups - 1) * cols)]
    pltpu.make_async_copy(rest, rest, res_recv).wait()
    for copy in sent + eg_copies + relays + res_copies:
        copy.wait_send()


def local(n, activations, out_grads, lengths, proj_in, proj_out, queries):
    tokens, ff = activations.shape
    d = out_grads.shape[1]
    rank = proj_in.shape[1]
    ex = lengths.shape[1]
    nq, params = queries.shape
    n_groups = n // GROUP
    slots = ROWS // ex
    bf16 = jnp.bfloat16
    dma = pltpu.SemaphoreType.DMA
    hbm = pl.BlockSpec(memory_space=pltpu.MemorySpace.HBM)
    return pl.pallas_call(
        functools.partial(kernel, n),
        out_shape=jax.ShapeDtypeStruct((ex, nq * n), bf16),
        in_specs=[hbm] * 6,
        out_specs=pl.BlockSpec(memory_space=pltpu.MemorySpace.VMEM),
        scratch_shapes=[
            pltpu.SMEM((1, ex), jnp.int32),
            pltpu.VMEM((tokens, ff), bf16),
            pltpu.VMEM((tokens, d), bf16),
            pltpu.VMEM((rank, ff), bf16),
            pltpu.VMEM((rank, d), bf16),
            pltpu.VMEM((GROUP, nq, params), bf16),
            pltpu.VMEM((n_groups, ex * params // LANES, LANES), bf16),
            pltpu.VMEM((n_groups, ex, GROUP * nq), bf16),
            pltpu.VMEM((2 * ex * params // LANES, tokens), bf16),
            dma((3,)),
            dma((PIECES,)),
            dma,
            dma,
            dma((slots,)),
            dma((slots,)),
            dma,
            dma,
        ],
        compiler_params=pltpu.CompilerParams(
            collective_id=0, has_side_effects=True, vmem_limit_bytes=56500000
        ),
    )(pltpu.with_memory_space_constraint(lengths, pltpu.HBM), activations, out_grads, proj_in.T, proj_out.T, queries)


def solution(mesh):
    in_specs = (
        P(("parts", "dp"), None),
        P(("parts", "dp"), None),
        P(("parts", "dp"), None),
        P(),
        P(),
        P(("parts", "dp"), None),
    )
    out_specs = P(("parts", "dp"), None)
    body = functools.partial(local, mesh.shape["dp"])
    return jax.shard_map(body, mesh=mesh, in_specs=in_specs, out_specs=out_specs, check_vma=False)
```

```python
import functools

import jax
import jax.numpy as jnp
from jax import lax
from jax.experimental import pallas as pl
from jax.experimental.pallas import tpu as pltpu
from jax.sharding import PartitionSpec as P

MESH = pl.DeviceIdType.MESH
NT = (((1,), (1,)), ((), ()))
NN = (((1,), (0,)), ((), ()))
GRAD_SHARES = (1,)
SHARES = (4, 4, 4, 4, 4, 4, 2, 1, 1)
EARLY = 0
AHEAD = 5
GROUP = 4
CORES = 2
LANES = 128
ROWS = 16


def kernel(
    n,
    lens_hbm,
    acts_hbm,
    grads_hbm,
    win_hbm,
    wout_hbm,
    q_hbm,
    out,
    lens,
    acts,
    grads,
    win,
    wout,
    q_own,
    qs,
    g_own,
    eg,
    stage,
    res,
    wide,
    gt,
    q_sem,
    grads_sem,
    acts_sem,
    send_sem,
    buddy_recv,
    across_recv,
    eg_recv,
    res_recv,
):
    me = lax.axis_index("dp")
    n_groups = n // GROUP
    group, lane = me // GROUP, lax.rem(me, GROUP)
    core = lax.rem(me, CORES)
    pair = lane - core
    far_pair = CORES - pair
    tokens, ff = acts.shape
    rank, d = wout.shape
    ex = stage.shape[1]
    slots = ROWS // ex
    nq, part = qs.shape[1:]
    span = part // slots
    tiles = span // LANES
    half = tiles * ROWS
    cols = GROUP * nq
    units = CORES * n_groups

    backward = (group < n_groups - group).astype(jnp.int32)

    def peer_group(t):
        return lax.rem(group + t + backward * (n_groups - 2 * t), n_groups)

    def device(g, c):
        return g * GROUP + pair + c

    buddy = device(group, 1 - core)
    across = [group * GROUP + far_pair + c for c in range(CORES)]

    def start(source, target, sem):
        load = pltpu.make_async_copy(source, target, sem)
        load.start()
        return load

    def cuts(size, shares):
        edges = [size * sum(shares[:p]) // sum(shares) for p in range(len(shares) + 1)]
        return list(zip(edges[:-1], edges[1:]))

    def fetch(rows_hbm, rows, weights_hbm, weights, sem, cut):
        side = pl.ds(cut[0], cut[1] - cut[0])
        return (
            start(weights_hbm.at[:, side], weights.at[:, side], sem),
            start(rows_hbm.at[:, side], rows.at[:, side], sem),
        )

    def project(sums, rows, weights, cut):
        for h in range(2):
            side = slice(h * tokens // 2, (h + 1) * tokens // 2)
            term = lax.dot_general(
                rows[side, cut[0] : cut[1]],
                weights[:, cut[0] : cut[1]],
                NT,
                preferred_element_type=jnp.float32,
            )
            sums[h] = term if sums[h] is None else sums[h] + term

    def send(source, target, recv_sem, other):
        copy = pltpu.make_async_remote_copy(
            src_ref=source,
            dst_ref=target,
            send_sem=send_sem,
            recv_sem=recv_sem,
            device_id={"dp": other},
            device_id_type=MESH,
        )
        copy.start()
        return copy

    mine = pl.ds(pl.multiple_of(core * part, LANES), part)
    load_q = start(q_hbm, q_own, q_sem)
    load_lens = start(lens_hbm, lens, grads_sem.at[0])
    grad_cuts, cut = cuts(d, GRAD_SHARES), cuts(ff, SHARES)
    load_grads = [
        fetch(grads_hbm, grads, wout_hbm, wout, grads_sem.at[p], grad_cuts[p])
        for p in range(len(grad_cuts))
    ]
    load_acts = {}

    def fetch_acts(p):
        if p < len(cut):
            load_acts[p] = fetch(acts_hbm, acts, win_hbm, win, acts_sem.at[p], cut[p])

    for p in range(EARLY):
        fetch_acts(p)

    barrier = pltpu.get_barrier_semaphore()
    column = [device(peer_group(t), c) for t in range(1, n_groups) for c in range(CORES)]
    partners = column + [buddy] + across
    for other in partners:
        pl.semaphore_signal(barrier, inc=1, device_id={"dp": other}, device_id_type=MESH)

    load_q.wait()
    for p in range(EARLY, AHEAD):
        fetch_acts(p)
    load_mine = start(q_hbm.at[:, mine], qs.at[lane], q_sem)
    pl.semaphore_wait(barrier, len(partners))
    copies = []
    for c in range(CORES):
        side = pl.ds(c * part, part)
        copies.append(send(q_own.at[:, side], qs.at[lane], across_recv, across[c]))
    other_half = pl.ds(pl.multiple_of((1 - core) * part, LANES), part)
    copies.append(send(q_own.at[:, other_half], qs.at[lane], buddy_recv, buddy))

    load_lens.wait()
    for load in load_grads[0]:
        load.wait()
    sums = [None, None]
    for p in range(len(grad_cuts)):
        if p > 0:
            for load in load_grads[p]:
                load.wait()
        project(sums, grads, wout, grad_cuts[p])
    token = lax.broadcasted_iota(jnp.int32, (8, tokens), 1)
    row_ex = lax.rem(lax.broadcasted_iota(jnp.int32, (8, tokens), 0), ex)
    first = jnp.int32(0)
    mask = jnp.zeros((8, tokens), jnp.float32)
    for e in range(ex):
        end = first + lens[0, e]
        mask = jnp.where((row_ex == e) & (token >= first) & (token < end), 1.0, mask)
        first = end
    gt[...] = jnp.concatenate(sums, axis=0).T

    at_row = lax.broadcasted_iota(jnp.int32, (8, tokens), 0)
    per_block = 8 // ex

    def widen(odd):
        for c, t in [(c, t) for c in range(CORES) for t in range(tiles)]:
            blocks = []
            for b in range(ROWS // 8):
                block = None
                for j in range(per_block):
                    s = b * per_block + j
                    row = 2 * ((c * slots + s) * tiles + t) + odd
                    one = jnp.broadcast_to(gt[row : row + 1], (8, tokens))
                    block = one if block is None else jnp.where(at_row >= j * ex, one, block)
                blocks.append(block * mask)
            at = c * half + t * ROWS
            wide[odd, at : at + ROWS] = jnp.concatenate(blocks, axis=0).astype(jnp.bfloat16)

    sums = [None, None]
    for p in range(len(cut)):
        for load in load_acts[p]:
            load.wait()
        fetch_acts(p + AHEAD)
        project(sums, acts, win, cut[p])
        if p < 2:
            widen(p)
    proj_acts = jnp.concatenate(sums, axis=0).astype(jnp.bfloat16)
    twice = jnp.concatenate([proj_acts, proj_acts], axis=1)
    even = lax.dot_general(wide[0], twice, NN, preferred_element_type=jnp.float32)
    odd = lax.dot_general(wide[1], twice, NN, preferred_element_type=jnp.float32)
    lower = lax.broadcasted_iota(jnp.int32, (CORES * half, 2 * rank), 1) < rank
    both = jnp.where(lower, even, odd).astype(jnp.bfloat16)
    for c in range(CORES):
        g_own[c] = both[c * half : (c + 1) * half]

    unit = group * CORES + core
    for t in range(1, n_groups):
        for c in range(CORES):
            copies.append(send(g_own.at[c], eg.at[unit], eg_recv, device(peer_group(t), c)))
    copies.append(send(g_own.at[1 - core], eg.at[unit], eg_recv, buddy))
    eg[unit] = g_own[core]

    load_mine.wait()
    copies[2].wait_recv()
    both_lanes = qs.at[pl.ds(far_pair, CORES)]
    pltpu.make_async_copy(both_lanes, both_lanes, across_recv).wait()
    rest = eg.at[pl.ds(0, units - 1)]
    pltpu.make_async_copy(rest, rest, eg_recv).wait()

    stacked = []
    for u in range(units):
        one = eg[u]
        stacked.append(
            jnp.concatenate([one[ROWS * t : ROWS * (t + 1)] for t in range(tiles)], axis=1)
        )
    stacked = jnp.concatenate(stacked, axis=0)
    scores = [None] * units
    for s in range(slots):
        queries = qs[:, :, s * span : (s + 1) * span].reshape(cols, span)
        term = lax.dot_general(stacked, queries, NT, preferred_element_type=jnp.float32)
        for u in range(units):
            row = ROWS * u + ex * s
            piece = term[row : row + ex]
            scores[u] = piece if scores[u] is None else scores[u] + piece
    for u in range(units):
        stage[u] = scores[u]

    slot = core * n_groups + group
    for t in range(1, n_groups):
        g = peer_group(t)
        for c in range(CORES):
            copies.append(send(stage.at[g * CORES + c], res.at[slot], res_recv, device(g, c)))
    copies.append(send(stage.at[group * CORES + 1 - core], res.at[slot], res_recv, buddy))
    res[slot] = stage[unit]
    rest = res.at[pl.ds(0, units - 1)]
    pltpu.make_async_copy(rest, rest, res_recv).wait()
    for g in range(n_groups):
        total = res[g] + res[n_groups + g]
        out[:, g * cols : (g + 1) * cols] = total.astype(jnp.bfloat16)
    for copy in copies:
        copy.wait_send()


def local(n, activations, out_grads, lengths, proj_in, proj_out, queries):
    tokens, ff = activations.shape
    d = out_grads.shape[1]
    rank = proj_in.shape[1]
    ex = lengths.shape[1]
    nq, params = queries.shape
    n_groups = n // GROUP
    units = CORES * n_groups
    rows = ex * params // LANES
    bf16, f32 = jnp.bfloat16, jnp.float32
    dma = pltpu.SemaphoreType.DMA
    hbm = pl.BlockSpec(memory_space=pltpu.MemorySpace.HBM)
    return pl.pallas_call(
        functools.partial(kernel, n),
        out_shape=jax.ShapeDtypeStruct((ex, nq * n), bf16),
        in_specs=[hbm] * 6,
        out_specs=pl.BlockSpec(memory_space=pltpu.MemorySpace.VMEM),
        scratch_shapes=[
            pltpu.SMEM((1, ex), jnp.int32),
            pltpu.VMEM((tokens, ff), bf16),
            pltpu.VMEM((tokens, d), bf16),
            pltpu.VMEM((rank, ff), bf16),
            pltpu.VMEM((rank, d), bf16),
            pltpu.VMEM((nq, params), bf16),
            pltpu.VMEM((GROUP, nq, params // CORES), bf16),
            pltpu.VMEM((CORES, rows // CORES, LANES), bf16),
            pltpu.VMEM((units, rows // CORES, LANES), bf16),
            pltpu.VMEM((units, ex, GROUP * nq), f32),
            pltpu.VMEM((units, ex, GROUP * nq), f32),
            pltpu.VMEM((2, rows, tokens), bf16),
            pltpu.VMEM((rank, tokens), f32),
            dma,
            dma((len(GRAD_SHARES),)),
            dma((len(SHARES),)),
            dma,
            dma,
            dma,
            dma,
            dma,
        ],
        compiler_params=pltpu.CompilerParams(
            collective_id=0, has_side_effects=True, vmem_limit_bytes=56500000
        ),
    )(pltpu.with_memory_space_constraint(lengths, pltpu.HBM), activations, out_grads, proj_in.T, proj_out.T, queries)


def solution(mesh):
    in_specs = (
        P(("parts", "dp"), None),
        P(("parts", "dp"), None),
        P(("parts", "dp"), None),
        P(),
        P(),
        P(("parts", "dp"), None),
    )
    out_specs = P(("parts", "dp"), None)
    body = functools.partial(local, mesh.shape["dp"])
    return jax.shard_map(body, mesh=mesh, in_specs=in_specs, out_specs=out_specs, check_vma=False)
```

```python
import functools

import jax
import jax.numpy as jnp
from jax import lax
from jax.experimental import pallas as pl
from jax.experimental.pallas import tpu as pltpu
from jax.sharding import PartitionSpec as P

MESH = pl.DeviceIdType.MESH
NT = (((1,), (1,)), ((), ()))
NN = (((1,), (0,)), ((), ()))
GRAD_SHARES = (1, 1)
SHARES = (4, 4, 4, 4, 4, 4, 2, 1, 1)
GROUP = 4
CORES = 2
LANES = 128
ROWS = 16


def kernel(
    n,
    lens_hbm,
    acts_hbm,
    grads_hbm,
    win_hbm,
    wout_hbm,
    q_hbm,
    out,
    lens,
    acts,
    grads,
    win,
    wout,
    q_own,
    qs,
    g_own,
    eg,
    stage,
    res,
    wide,
    gt,
    q_sem,
    grads_sem,
    acts_sem,
    send_sem,
    buddy_recv,
    across_recv,
    eg_recv,
    res_recv,
):
    me = lax.axis_index("dp")
    n_groups = n // GROUP
    group, lane = me // GROUP, lax.rem(me, GROUP)
    core = lax.rem(me, CORES)
    pair = lane - core
    far_pair = CORES - pair
    tokens, ff = acts.shape
    rank, d = wout.shape
    ex = stage.shape[1]
    slots = ROWS // ex
    nq, part = qs.shape[1:]
    span = part // slots
    tiles = span // LANES
    half = tiles * ROWS
    cols = GROUP * nq
    units = CORES * n_groups

    backward = (group < n_groups - group).astype(jnp.int32)

    def peer_group(t):
        return lax.rem(group + t + backward * (n_groups - 2 * t), n_groups)

    def device(g, c):
        return g * GROUP + pair + c

    buddy = device(group, 1 - core)
    across = [group * GROUP + far_pair + c for c in range(CORES)]

    def start(source, target, sem):
        load = pltpu.make_async_copy(source, target, sem)
        load.start()
        return load

    def cuts(size, shares):
        edges = [size * sum(shares[:p]) // sum(shares) for p in range(len(shares) + 1)]
        return list(zip(edges[:-1], edges[1:]))

    def fetch(rows_hbm, rows, weights_hbm, weights, sem, cut):
        side = pl.ds(cut[0], cut[1] - cut[0])
        return (
            start(weights_hbm.at[:, side], weights.at[:, side], sem),
            start(rows_hbm.at[:, side], rows.at[:, side], sem),
        )

    def project(sums, rows, weights, cut):
        for h in range(2):
            side = slice(h * tokens // 2, (h + 1) * tokens // 2)
            term = lax.dot_general(
                rows[side, cut[0] : cut[1]],
                weights[:, cut[0] : cut[1]],
                NT,
                preferred_element_type=jnp.float32,
            )
            sums[h] = term if sums[h] is None else sums[h] + term

    def remote(source, target, recv_sem, other):
        return pltpu.make_async_remote_copy(
            src_ref=source,
            dst_ref=target,
            send_sem=send_sem,
            recv_sem=recv_sem,
            device_id={"dp": other},
            device_id_type=MESH,
        )

    def send(source, target, recv_sem, other):
        copy = remote(source, target, recv_sem, other)
        copy.start()
        return copy

    mine = pl.ds(pl.multiple_of(core * part, LANES), part)
    barrier = pltpu.get_barrier_semaphore()
    column = [device(peer_group(t), c) for t in range(1, n_groups) for c in range(CORES)]
    partners = across + [buddy] + column
    waiting = list(partners)

    def announce(count):
        for other in waiting[:count]:
            pl.semaphore_signal(barrier, inc=1, device_id={"dp": other}, device_id_type=MESH)
        del waiting[:count]

    grad_cuts, cut = cuts(d, GRAD_SHARES), cuts(ff, SHARES)
    load_q = start(q_hbm, q_own, q_sem)
    announce(3)
    load_lens = start(lens_hbm, lens, grads_sem.at[0])
    load_grads, load_acts = [], []
    for p in range(len(grad_cuts)):
        load_grads.append(fetch(grads_hbm, grads, wout_hbm, wout, grads_sem.at[p], grad_cuts[p]))
        announce(1)
    for p in range(len(cut)):
        load_acts.append(fetch(acts_hbm, acts, win_hbm, win, acts_sem.at[p], cut[p]))
        announce(1)
    announce(len(waiting))

    load_q.wait()
    other_half = pl.ds(pl.multiple_of((1 - core) * part, LANES), part)
    copies = [
        remote(q_own.at[:, pl.ds(c * part, part)], qs.at[lane], across_recv, across[c])
        for c in range(CORES)
    ]
    copies.append(remote(q_own.at[:, other_half], qs.at[lane], buddy_recv, buddy))

    def meet():
        pl.semaphore_wait(barrier, len(partners))
        for copy in copies[:3]:
            copy.start()

    lower_half = group < n_groups // 2
    pl.when(jnp.logical_not(lower_half))(meet)
    load_mine = start(q_hbm.at[:, mine], qs.at[lane], q_sem)

    load_lens.wait()
    for load in load_grads[0]:
        load.wait()
    sums = [None, None]
    for p in range(len(grad_cuts)):
        if p > 0:
            for load in load_grads[p]:
                load.wait()
        project(sums, grads, wout, grad_cuts[p])
    token = lax.broadcasted_iota(jnp.int32, (8, tokens), 1)
    row_ex = lax.rem(lax.broadcasted_iota(jnp.int32, (8, tokens), 0), ex)
    first = jnp.int32(0)
    mask = jnp.zeros((8, tokens), jnp.float32)
    for e in range(ex):
        end = first + lens[0, e]
        mask = jnp.where((row_ex == e) & (token >= first) & (token < end), 1.0, mask)
        first = end
    gt[...] = jnp.concatenate(sums, axis=0).T

    at_row = lax.broadcasted_iota(jnp.int32, (8, tokens), 0)
    per_block = 8 // ex

    def widen(odd):
        for c, t in [(c, t) for c in range(CORES) for t in range(tiles)]:
            blocks = []
            for b in range(ROWS // 8):
                block = None
                for j in range(per_block):
                    s = b * per_block + j
                    row = 2 * ((c * slots + s) * tiles + t) + odd
                    one = jnp.broadcast_to(gt[row : row + 1], (8, tokens))
                    block = one if block is None else jnp.where(at_row >= j * ex, one, block)
                blocks.append(block * mask)
            at = c * half + t * ROWS
            wide[odd, at : at + ROWS] = jnp.concatenate(blocks, axis=0).astype(jnp.bfloat16)

    pl.when(lower_half)(meet)
    sums = [None, None]
    for p in range(len(cut)):
        for load in load_acts[p]:
            load.wait()
        project(sums, acts, win, cut[p])
        if p < 2:
            widen(p)
    proj_acts = jnp.concatenate(sums, axis=0).astype(jnp.bfloat16)
    twice = jnp.concatenate([proj_acts, proj_acts], axis=1)
    even = lax.dot_general(wide[0], twice, NN, preferred_element_type=jnp.float32)
    odd = lax.dot_general(wide[1], twice, NN, preferred_element_type=jnp.float32)
    lower = lax.broadcasted_iota(jnp.int32, (CORES * half, 2 * rank), 1) < rank
    both = jnp.where(lower, even, odd).astype(jnp.bfloat16)
    for c in range(CORES):
        g_own[c] = both[c * half : (c + 1) * half]

    unit = group * CORES + core
    for t in range(1, n_groups):
        for c in range(CORES):
            copies.append(send(g_own.at[c], eg.at[unit], eg_recv, device(peer_group(t), c)))
    copies.append(send(g_own.at[1 - core], eg.at[unit], eg_recv, buddy))
    eg[unit] = g_own[core]

    load_mine.wait()
    copies[2].wait_recv()
    both_lanes = qs.at[pl.ds(far_pair, CORES)]
    pltpu.make_async_copy(both_lanes, both_lanes, across_recv).wait()
    rest = eg.at[pl.ds(0, units - 1)]
    pltpu.make_async_copy(rest, rest, eg_recv).wait()

    stacked = []
    for u in range(units):
        one = eg[u]
        stacked.append(
            jnp.concatenate([one[ROWS * t : ROWS * (t + 1)] for t in range(tiles)], axis=1)
        )
    stacked = jnp.concatenate(stacked, axis=0)
    scores = [None] * units
    for s in range(slots):
        queries = qs[:, :, s * span : (s + 1) * span].reshape(cols, span)
        term = lax.dot_general(stacked, queries, NT, preferred_element_type=jnp.float32)
        for u in range(units):
            row = ROWS * u + ex * s
            piece = term[row : row + ex]
            scores[u] = piece if scores[u] is None else scores[u] + piece
    for u in range(units):
        stage[u] = scores[u]

    slot = core * n_groups + group
    for t in range(1, n_groups):
        g = peer_group(t)
        for c in range(CORES):
            copies.append(send(stage.at[g * CORES + c], res.at[slot], res_recv, device(g, c)))
    copies.append(send(stage.at[group * CORES + 1 - core], res.at[slot], res_recv, buddy))
    res[slot] = stage[unit]
    rest = res.at[pl.ds(0, units - 1)]
    pltpu.make_async_copy(rest, rest, res_recv).wait()
    for g in range(n_groups):
        total = res[g] + res[n_groups + g]
        out[:, g * cols : (g + 1) * cols] = total.astype(jnp.bfloat16)
    for copy in copies:
        copy.wait_send()


def local(n, activations, out_grads, lengths, proj_in, proj_out, queries):
    tokens, ff = activations.shape
    d = out_grads.shape[1]
    rank = proj_in.shape[1]
    ex = lengths.shape[1]
    nq, params = queries.shape
    n_groups = n // GROUP
    units = CORES * n_groups
    rows = ex * params // LANES
    bf16, f32 = jnp.bfloat16, jnp.float32
    dma = pltpu.SemaphoreType.DMA
    hbm = pl.BlockSpec(memory_space=pltpu.MemorySpace.HBM)
    return pl.pallas_call(
        functools.partial(kernel, n),
        out_shape=jax.ShapeDtypeStruct((ex, nq * n), bf16),
        in_specs=[hbm] * 6,
        out_specs=pl.BlockSpec(memory_space=pltpu.MemorySpace.VMEM),
        scratch_shapes=[
            pltpu.SMEM((1, ex), jnp.int32),
            pltpu.VMEM((tokens, ff), bf16),
            pltpu.VMEM((tokens, d), bf16),
            pltpu.VMEM((rank, ff), bf16),
            pltpu.VMEM((rank, d), bf16),
            pltpu.VMEM((nq, params), bf16),
            pltpu.VMEM((GROUP, nq, params // CORES), bf16),
            pltpu.VMEM((CORES, rows // CORES, LANES), bf16),
            pltpu.VMEM((units, rows // CORES, LANES), bf16),
            pltpu.VMEM((units, ex, GROUP * nq), f32),
            pltpu.VMEM((units, ex, GROUP * nq), f32),
            pltpu.VMEM((2, rows, tokens), bf16),
            pltpu.VMEM((rank, tokens), f32),
            dma,
            dma((len(GRAD_SHARES),)),
            dma((len(SHARES),)),
            dma,
            dma,
            dma,
            dma,
            dma,
        ],
        compiler_params=pltpu.CompilerParams(
            collective_id=0, has_side_effects=True, vmem_limit_bytes=56500000
        ),
    )(pltpu.with_memory_space_constraint(lengths, pltpu.HBM), activations, out_grads, proj_in.T, proj_out.T, queries)


def solution(mesh):
    in_specs = (
        P(("parts", "dp"), None),
        P(("parts", "dp"), None),
        P(("parts", "dp"), None),
        P(),
        P(),
        P(("parts", "dp"), None),
    )
    out_specs = P(("parts", "dp"), None)
    body = functools.partial(local, mesh.shape["dp"])
    return jax.shard_map(body, mesh=mesh, in_specs=in_specs, out_specs=out_specs, check_vma=False)
```

```python
import functools

import jax
import jax.numpy as jnp
from jax import lax
from jax.experimental import pallas as pl
from jax.experimental.pallas import tpu as pltpu
from jax.sharding import PartitionSpec as P

MESH = pl.DeviceIdType.MESH
NT = (((1,), (1,)), ((), ()))
NN = (((1,), (0,)), ((), ()))
GRAD_SHARES = (1, 1)
SHARES = (4, 6, 6, 6, 4, 2)
GROUP = 4
CORES = 2
LANES = 128
ROWS = 16


def kernel(
    n,
    lens_hbm,
    acts_hbm,
    grads_hbm,
    win_hbm,
    wout_hbm,
    q_hbm,
    out,
    lens,
    acts,
    grads,
    win,
    wout,
    q_own,
    qs,
    g_own,
    eg,
    stage,
    res,
    wide,
    gt,
    q_sem,
    grads_sem,
    acts_sem,
    send_sem,
    q_recv,
    eg_recv,
    res_recv,
):
    me = lax.axis_index("dp")
    n_groups = n // GROUP
    group, lane = me // GROUP, lax.rem(me, GROUP)
    core = lax.rem(me, CORES)
    pair = lane - core
    far_pair = CORES - pair
    tokens, ff = acts.shape
    rank, d = wout.shape
    ex = stage.shape[1]
    slots = ROWS // ex
    nq, part = qs.shape[1:]
    span = part // slots
    tiles = span // LANES
    half = tiles * ROWS
    cols = GROUP * nq
    units = CORES * n_groups

    backward = (group < n_groups - group).astype(jnp.int32)

    def peer_group(t):
        return lax.rem(group + t + backward * (n_groups - 2 * t), n_groups)

    def device(g, c):
        return g * GROUP + pair + c

    buddy = device(group, 1 - core)
    across = [group * GROUP + far_pair + c for c in range(CORES)]

    def start(source, target, sem):
        load = pltpu.make_async_copy(source, target, sem)
        load.start()
        return load

    def cuts(size, shares):
        edges = [size * sum(shares[:p]) // sum(shares) for p in range(len(shares) + 1)]
        return list(zip(edges[:-1], edges[1:]))

    def fetch(rows_hbm, rows, weights_hbm, weights, sem, cut):
        side = pl.ds(cut[0], cut[1] - cut[0])
        return (
            start(weights_hbm.at[:, side], weights.at[:, side], sem),
            start(rows_hbm.at[:, side], rows.at[:, side], sem),
        )

    def project(sums, rows, weights, cut):
        for h in range(2):
            side = slice(h * tokens // 2, (h + 1) * tokens // 2)
            term = lax.dot_general(
                rows[side, cut[0] : cut[1]],
                weights[:, cut[0] : cut[1]],
                NT,
                preferred_element_type=jnp.float32,
            )
            sums[h] = term if sums[h] is None else sums[h] + term

    def remote(source, target, recv_sem, other):
        return pltpu.make_async_remote_copy(
            src_ref=source,
            dst_ref=target,
            send_sem=send_sem,
            recv_sem=recv_sem,
            device_id={"dp": other},
            device_id_type=MESH,
        )

    def send(source, target, recv_sem, other):
        copy = remote(source, target, recv_sem, other)
        copy.start()
        return copy

    mine = pl.ds(pl.multiple_of(core * part, LANES), part)
    barrier = pltpu.get_barrier_semaphore()
    column = [device(peer_group(t), c) for t in range(1, n_groups) for c in range(CORES)]
    partners = across + [buddy] + column
    waiting = list(partners)

    def announce(count):
        for other in waiting[:count]:
            pl.semaphore_signal(barrier, inc=1, device_id={"dp": other}, device_id_type=MESH)
        del waiting[:count]

    grad_cuts, cut = cuts(d, GRAD_SHARES), cuts(ff, SHARES)
    load_q = start(q_hbm, q_own, q_sem)
    announce(3)
    load_lens = start(lens_hbm, lens, grads_sem.at[0])
    load_grads, load_acts = [], []
    for p in range(len(grad_cuts)):
        load_grads.append(fetch(grads_hbm, grads, wout_hbm, wout, grads_sem.at[p], grad_cuts[p]))
        announce(1)
    for p in range(len(cut)):
        load_acts.append(fetch(acts_hbm, acts, win_hbm, win, acts_sem.at[p], cut[p]))
        announce(1)
    announce(len(waiting))

    load_q.wait()
    other_half = pl.ds(pl.multiple_of((1 - core) * part, LANES), part)
    copies = [
        remote(q_own.at[:, pl.ds(c * part, part)], qs.at[lane], q_recv, across[c])
        for c in range(CORES)
    ]
    copies.append(remote(q_own.at[:, other_half], qs.at[lane], q_recv, buddy))

    def meet():
        pl.semaphore_wait(barrier, len(partners))
        for copy in copies[:3]:
            copy.start()

    lower_half = group < n_groups // 2
    load_mine = start(q_hbm.at[:, mine], qs.at[lane], q_sem)

    at_row = lax.broadcasted_iota(jnp.int32, (8, tokens), 0)
    per_block = 8 // ex

    def masks():
        token = lax.broadcasted_iota(jnp.int32, (8, tokens), 1)
        row_ex = lax.rem(at_row, ex)
        begin = jnp.int32(0)
        mask = jnp.zeros((8, tokens), jnp.float32)
        for e in range(ex):
            end = begin + lens[0, e]
            mask = jnp.where((row_ex == e) & (token >= begin) & (token < end), 1.0, mask)
            begin = end
        return mask

    def widen(odd, mask):
        for c, t in [(c, t) for c in range(CORES) for t in range(tiles)]:
            blocks = []
            for b in range(ROWS // 8):
                block = None
                for j in range(per_block):
                    s = b * per_block + j
                    row = 2 * ((c * slots + s) * tiles + t) + odd
                    one = jnp.broadcast_to(gt[row : row + 1], (8, tokens))
                    block = one if block is None else jnp.where(at_row >= j * ex, one, block)
                blocks.append(block * mask)
            at = c * half + t * ROWS
            wide[odd, at : at + ROWS] = jnp.concatenate(blocks, axis=0).astype(jnp.bfloat16)

    def produce(meet_late):
        if not meet_late:
            meet()
        load_lens.wait()
        of_grads = [None, None]
        for p in range(len(grad_cuts)):
            for load in load_grads[p]:
                load.wait()
            project(of_grads, grads, wout, grad_cuts[p])

        def keep():
            gt[...] = jnp.concatenate(of_grads, axis=0).T

        if meet_late:
            keep()
            meet()
        of_acts = [None, None]
        for p in range(len(cut)):
            for load in load_acts[p]:
                load.wait()
            project(of_acts, acts, win, cut[p])
            if p == 0 and not meet_late:
                keep()
            if p == 1:
                mask = masks()
                widen(0, mask)
            if p == 2:
                widen(1, mask)
        proj_acts = jnp.concatenate(of_acts, axis=0).astype(jnp.bfloat16)
        twice = jnp.concatenate([proj_acts, proj_acts], axis=1)
        even = lax.dot_general(wide[0], twice, NN, preferred_element_type=jnp.float32)
        odd = lax.dot_general(wide[1], twice, NN, preferred_element_type=jnp.float32)
        lower = lax.broadcasted_iota(jnp.int32, (CORES * half, 2 * rank), 1) < rank
        both = jnp.where(lower, even, odd).astype(jnp.bfloat16)
        for c in range(CORES):
            g_own[c] = both[c * half : (c + 1) * half]

    pl.when(lower_half)(lambda: produce(True))
    pl.when(jnp.logical_not(lower_half))(lambda: produce(False))

    unit = group * CORES + core
    for c in range(CORES):
        for t in range(1, n_groups):
            copies.append(send(g_own.at[c], eg.at[unit], eg_recv, device(peer_group(t), c)))
    copies.append(send(g_own.at[1 - core], eg.at[unit], eg_recv, buddy))
    eg[unit] = g_own[core]

    load_mine.wait()
    others = qs.at[pl.ds(0, GROUP - 1)]
    pltpu.make_async_copy(others, others, q_recv).wait()
    rest = eg.at[pl.ds(0, units - 1)]
    pltpu.make_async_copy(rest, rest, eg_recv).wait()

    stacked = []
    for u in range(units):
        one = eg[u]
        stacked.append(
            jnp.concatenate([one[ROWS * t : ROWS * (t + 1)] for t in range(tiles)], axis=1)
        )
    stacked = jnp.concatenate(stacked, axis=0)
    scores = [None] * units
    for s in range(slots):
        queries = qs[:, :, s * span : (s + 1) * span].reshape(cols, span)
        term = lax.dot_general(stacked, queries, NT, preferred_element_type=jnp.float32)
        for u in range(units):
            row = ROWS * u + ex * s
            piece = term[row : row + ex]
            scores[u] = piece if scores[u] is None else scores[u] + piece
    for u in range(units):
        stage[u] = scores[u]

    slot = core * n_groups + group
    for t in range(1, n_groups):
        g = peer_group(t)
        for c in range(CORES):
            copies.append(send(stage.at[g * CORES + c], res.at[slot], res_recv, device(g, c)))
    copies.append(send(stage.at[group * CORES + 1 - core], res.at[slot], res_recv, buddy))
    res[slot] = stage[unit]
    rest = res.at[pl.ds(0, units - 1)]
    pltpu.make_async_copy(rest, rest, res_recv).wait()
    for g in range(n_groups):
        total = res[g] + res[n_groups + g]
        out[:, g * cols : (g + 1) * cols] = total.astype(jnp.bfloat16)
    for copy in copies:
        copy.wait_send()


def local(n, activations, out_grads, lengths, proj_in, proj_out, queries):
    tokens, ff = activations.shape
    d = out_grads.shape[1]
    rank = proj_in.shape[1]
    ex = lengths.shape[1]
    nq, params = queries.shape
    n_groups = n // GROUP
    units = CORES * n_groups
    rows = ex * params // LANES
    bf16, f32 = jnp.bfloat16, jnp.float32
    dma = pltpu.SemaphoreType.DMA
    hbm = pl.BlockSpec(memory_space=pltpu.MemorySpace.HBM)
    return pl.pallas_call(
        functools.partial(kernel, n),
        out_shape=jax.ShapeDtypeStruct((ex, nq * n), bf16),
        in_specs=[hbm] * 6,
        out_specs=pl.BlockSpec(memory_space=pltpu.MemorySpace.VMEM),
        scratch_shapes=[
            pltpu.SMEM((1, ex), jnp.int32),
            pltpu.VMEM((tokens, ff), bf16),
            pltpu.VMEM((tokens, d), bf16),
            pltpu.VMEM((rank, ff), bf16),
            pltpu.VMEM((rank, d), bf16),
            pltpu.VMEM((nq, params), bf16),
            pltpu.VMEM((GROUP, nq, params // CORES), bf16),
            pltpu.VMEM((CORES, rows // CORES, LANES), bf16),
            pltpu.VMEM((units, rows // CORES, LANES), bf16),
            pltpu.VMEM((units, ex, GROUP * nq), f32),
            pltpu.VMEM((units, ex, GROUP * nq), f32),
            pltpu.VMEM((2, rows, tokens), bf16),
            pltpu.VMEM((rank, tokens), f32),
            dma,
            dma((len(GRAD_SHARES),)),
            dma((len(SHARES),)),
            dma,
            dma,
            dma,
            dma,
        ],
        compiler_params=pltpu.CompilerParams(
            collective_id=0, has_side_effects=True, vmem_limit_bytes=56500000
        ),
    )(pltpu.with_memory_space_constraint(lengths, pltpu.HBM), activations, out_grads, proj_in.T, proj_out.T, queries)


def solution(mesh):
    in_specs = (
        P(("parts", "dp"), None),
        P(("parts", "dp"), None),
        P(("parts", "dp"), None),
        P(),
        P(),
        P(("parts", "dp"), None),
    )
    out_specs = P(("parts", "dp"), None)
    body = functools.partial(local, mesh.shape["dp"])
    return jax.shard_map(body, mesh=mesh, in_specs=in_specs, out_specs=out_specs, check_vma=False)
```

```python
import functools

import jax
import jax.numpy as jnp
from jax import lax
from jax.experimental import pallas as pl
from jax.experimental.pallas import tpu as pltpu
from jax.sharding import PartitionSpec as P

MESH = pl.DeviceIdType.MESH
NT = (((1,), (1,)), ((), ()))
NN = (((1,), (0,)), ((), ()))
GRAD_SHARES = (1, 1)
SHARES = (4, 6, 6, 6, 4, 2)
GROUP = 4
CORES = 2
LANES = 128
ROWS = 16


def kernel(
    n,
    lens_hbm,
    acts_hbm,
    grads_hbm,
    win_hbm,
    wout_hbm,
    q_hbm,
    res,
    lens,
    acts,
    grads,
    win,
    wout,
    q_own,
    qs,
    g_own,
    eg,
    stage,
    wide,
    gt,
    q_sem,
    grads_sem,
    acts_sem,
    send_sem,
    q_recv,
    eg_recv,
    res_recv,
):
    me = lax.axis_index("dp")
    n_groups = n // GROUP
    group, lane = me // GROUP, lax.rem(me, GROUP)
    core = lax.rem(me, CORES)
    pair = lane - core
    far_pair = CORES - pair
    tokens, ff = acts.shape
    rank, d = wout.shape
    ex = stage.shape[1]
    slots = ROWS // ex
    nq, part = qs.shape[1:]
    span = part // slots
    tiles = span // LANES
    half = tiles * ROWS
    cols = GROUP * nq
    units = CORES * n_groups

    backward = (group < n_groups - group).astype(jnp.int32)

    def peer_group(t):
        return lax.rem(group + t + backward * (n_groups - 2 * t), n_groups)

    def device(g, c):
        return g * GROUP + pair + c

    buddy = device(group, 1 - core)
    across = [group * GROUP + far_pair + c for c in range(CORES)]

    def start(source, target, sem):
        load = pltpu.make_async_copy(source, target, sem)
        load.start()
        return load

    def cuts(size, shares):
        edges = [size * sum(shares[:p]) // sum(shares) for p in range(len(shares) + 1)]
        return list(zip(edges[:-1], edges[1:]))

    def fetch(rows_hbm, rows, weights_hbm, weights, sem, cut):
        side = pl.ds(cut[0], cut[1] - cut[0])
        return (
            start(weights_hbm.at[:, side], weights.at[:, side], sem),
            start(rows_hbm.at[:, side], rows.at[:, side], sem),
        )

    def project(sums, rows, weights, cut):
        for h in range(2):
            side = slice(h * tokens // 2, (h + 1) * tokens // 2)
            term = lax.dot_general(
                rows[side, cut[0] : cut[1]],
                weights[:, cut[0] : cut[1]],
                NT,
                preferred_element_type=jnp.float32,
            )
            sums[h] = term if sums[h] is None else sums[h] + term

    def remote(source, target, recv_sem, other):
        return pltpu.make_async_remote_copy(
            src_ref=source,
            dst_ref=target,
            send_sem=send_sem,
            recv_sem=recv_sem,
            device_id={"dp": other},
            device_id_type=MESH,
        )

    def send(source, target, recv_sem, other):
        copy = remote(source, target, recv_sem, other)
        copy.start()
        return copy

    mine = pl.ds(pl.multiple_of(core * part, LANES), part)
    barrier = pltpu.get_barrier_semaphore()
    column = [device(peer_group(t), c) for t in range(1, n_groups) for c in range(CORES)]
    partners = across + [buddy] + column
    waiting = list(partners)

    def announce(count):
        for other in waiting[:count]:
            pl.semaphore_signal(barrier, inc=1, device_id={"dp": other}, device_id_type=MESH)
        del waiting[:count]

    grad_cuts, cut = cuts(d, GRAD_SHARES), cuts(ff, SHARES)
    load_q = start(q_hbm, q_own, q_sem)
    announce(3)
    load_lens = start(lens_hbm, lens, grads_sem.at[0])
    load_grads, load_acts = [], []
    for p in range(len(grad_cuts)):
        load_grads.append(fetch(grads_hbm, grads, wout_hbm, wout, grads_sem.at[p], grad_cuts[p]))
        announce(1)
    for p in range(len(cut)):
        load_acts.append(fetch(acts_hbm, acts, win_hbm, win, acts_sem.at[p], cut[p]))
        announce(1)
    announce(len(waiting))

    load_q.wait()
    other_half = pl.ds(pl.multiple_of((1 - core) * part, LANES), part)
    copies = [
        remote(q_own.at[:, pl.ds(c * part, part)], qs.at[lane], q_recv, across[c])
        for c in range(CORES)
    ]
    copies.append(remote(q_own.at[:, other_half], qs.at[lane], q_recv, buddy))

    def meet():
        pl.semaphore_wait(barrier, len(partners))
        for copy in copies[:3]:
            copy.start()

    lower_half = group < n_groups // 2
    load_mine = start(q_hbm.at[:, mine], qs.at[lane], q_sem)

    at_row = lax.broadcasted_iota(jnp.int32, (8, tokens), 0)
    per_block = 8 // ex

    def masks():
        token = lax.broadcasted_iota(jnp.int32, (8, tokens), 1)
        row_ex = lax.rem(at_row, ex)
        begin = jnp.int32(0)
        mask = jnp.zeros((8, tokens), jnp.float32)
        for e in range(ex):
            end = begin + lens[0, e]
            mask = jnp.where((row_ex == e) & (token >= begin) & (token < end), 1.0, mask)
            begin = end
        return mask

    def widen(odd, mask):
        for c, t in [(c, t) for c in range(CORES) for t in range(tiles)]:
            blocks = []
            for b in range(ROWS // 8):
                block = None
                for j in range(per_block):
                    s = b * per_block + j
                    row = 2 * ((c * slots + s) * tiles + t) + odd
                    one = jnp.broadcast_to(gt[row : row + 1], (8, tokens))
                    block = one if block is None else jnp.where(at_row >= j * ex, one, block)
                blocks.append(block * mask)
            at = c * half + t * ROWS
            wide[odd, at : at + ROWS] = jnp.concatenate(blocks, axis=0).astype(jnp.bfloat16)

    def produce(meet_late):
        if not meet_late:
            meet()
        load_lens.wait()
        of_grads = [None, None]
        for p in range(len(grad_cuts)):
            for load in load_grads[p]:
                load.wait()
            project(of_grads, grads, wout, grad_cuts[p])

        def keep():
            gt[...] = jnp.concatenate(of_grads, axis=0).T

        if meet_late:
            keep()
            pl.when(me >= CORES)(meet)
        of_acts = [None, None]
        for p in range(len(cut)):
            for load in load_acts[p]:
                load.wait()
            project(of_acts, acts, win, cut[p])
            if p == 0 and not meet_late:
                keep()
            if p == 1:
                mask = masks()
                widen(0, mask)
            if p == 2:
                widen(1, mask)
        proj_acts = jnp.concatenate(of_acts, axis=0).astype(jnp.bfloat16)
        twice = jnp.concatenate([proj_acts, proj_acts], axis=1)
        even = lax.dot_general(wide[0], twice, NN, preferred_element_type=jnp.float32)
        odd = lax.dot_general(wide[1], twice, NN, preferred_element_type=jnp.float32)
        lower = lax.broadcasted_iota(jnp.int32, (CORES * half, 2 * rank), 1) < rank
        both = jnp.where(lower, even, odd).astype(jnp.bfloat16)
        for c in range(CORES):
            g_own[c] = both[c * half : (c + 1) * half]

    pl.when(lower_half)(lambda: produce(True))
    pl.when(jnp.logical_not(lower_half))(lambda: produce(False))

    pl.when(me < CORES)(meet)
    unit = group * CORES + core
    home = group == 0
    away = jnp.logical_not(home)
    kind = jnp.where(home, 0, 1)
    for c in range(CORES):
        for t in range(1, n_groups):
            copies.append(send(g_own.at[c], eg.at[unit], eg_recv.at[kind], device(peer_group(t), c)))
    copies.append(send(g_own.at[1 - core], eg.at[unit], eg_recv.at[kind], buddy))
    eg[unit] = g_own[core]

    load_mine.wait()
    others = qs.at[pl.ds(0, GROUP - 1)]
    pltpu.make_async_copy(others, others, q_recv).wait()
    slot = core * n_groups + group

    def arrived(count, sem):
        block = eg.at[pl.ds(0, count)]
        pltpu.make_async_copy(block, block, sem).wait()

    def score(low, high):
        stacked = []
        for u in range(low, high):
            one = eg[u]
            stacked.append(
                jnp.concatenate([one[ROWS * t : ROWS * (t + 1)] for t in range(tiles)], axis=1)
            )
        stacked = jnp.concatenate(stacked, axis=0)
        scores = [None] * (high - low)
        for s in range(slots):
            queries = qs[:, :, s * span : (s + 1) * span].reshape(cols, span)
            term = lax.dot_general(stacked, queries, NT, preferred_element_type=jnp.float32)
            for u in range(high - low):
                row = ROWS * u + ex * s
                piece = term[row : row + ex]
                scores[u] = piece if scores[u] is None else scores[u] + piece
        for u in range(low, high):
            stage[u] = scores[u - low]

    def deliver(u, other):
        return remote(stage.at[u], res.at[slot], res_recv, other)

    to_buddy = deliver(group * CORES + 1 - core, buddy)
    to_home = [deliver(c, device(0, c)) for c in range(CORES)]
    onward = []
    for t in range(1, n_groups):
        g = peer_group(t)
        for c in range(CORES):
            onward.append((g > 0, deliver(g * CORES + c, device(g, c))))

    def settle():
        to_buddy.start()
        res[slot] = stage[unit]

    pl.when(home)(lambda: arrived(1, eg_recv.at[0]))
    pl.when(away)(lambda: arrived(CORES, eg_recv.at[0]))
    score(0, CORES)
    pl.when(home)(settle)

    @pl.when(away)
    def _():
        for copy in to_home:
            copy.start()

    pl.when(home)(lambda: arrived(units - CORES, eg_recv.at[1]))
    pl.when(away)(lambda: arrived(units - CORES - 1, eg_recv.at[1]))
    score(CORES, units)
    for wanted, copy in onward:
        pl.when(wanted)(copy.start)
    pl.when(away)(settle)
    rest = res.at[pl.ds(0, units - 1)]
    pltpu.make_async_copy(rest, rest, res_recv).wait()
    for copy in copies + [to_buddy]:
        copy.wait_send()

    @pl.when(away)
    def _():
        for copy in to_home:
            copy.wait_send()

    for wanted, copy in onward:
        pl.when(wanted)(copy.wait_send)


def local(n, activations, out_grads, lengths, proj_in, proj_out, queries):
    tokens, ff = activations.shape
    d = out_grads.shape[1]
    rank = proj_in.shape[1]
    ex = lengths.shape[1]
    nq, params = queries.shape
    n_groups = n // GROUP
    units = CORES * n_groups
    rows = ex * params // LANES
    bf16, f32 = jnp.bfloat16, jnp.float32
    dma = pltpu.SemaphoreType.DMA
    hbm = pl.BlockSpec(memory_space=pltpu.MemorySpace.HBM)
    parts = pl.pallas_call(
        functools.partial(kernel, n),
        out_shape=jax.ShapeDtypeStruct((units, ex, GROUP * nq), f32),
        in_specs=[hbm] * 6,
        out_specs=pl.BlockSpec(memory_space=pltpu.MemorySpace.VMEM),
        scratch_shapes=[
            pltpu.SMEM((1, ex), jnp.int32),
            pltpu.VMEM((tokens, ff), bf16),
            pltpu.VMEM((tokens, d), bf16),
            pltpu.VMEM((rank, ff), bf16),
            pltpu.VMEM((rank, d), bf16),
            pltpu.VMEM((nq, params), bf16),
            pltpu.VMEM((GROUP, nq, params // CORES), bf16),
            pltpu.VMEM((CORES, rows // CORES, LANES), bf16),
            pltpu.VMEM((units, rows // CORES, LANES), bf16),
            pltpu.VMEM((units, ex, GROUP * nq), f32),
            pltpu.VMEM((2, rows, tokens), bf16),
            pltpu.VMEM((rank, tokens), f32),
            dma,
            dma((len(GRAD_SHARES),)),
            dma((len(SHARES),)),
            dma,
            dma,
            dma((2,)),
            dma,
        ],
        compiler_params=pltpu.CompilerParams(
            collective_id=0, has_side_effects=True, vmem_limit_bytes=56500000
        ),
    )(pltpu.with_memory_space_constraint(lengths, pltpu.HBM), activations, out_grads, proj_in.T, proj_out.T, queries)
    total = parts[:n_groups] + parts[n_groups:]
    return total.swapaxes(0, 1).reshape(ex, nq * n).astype(bf16)


def solution(mesh):
    in_specs = (
        P(("parts", "dp"), None),
        P(("parts", "dp"), None),
        P(("parts", "dp"), None),
        P(),
        P(),
        P(("parts", "dp"), None),
    )
    out_specs = P(("parts", "dp"), None)
    body = functools.partial(local, mesh.shape["dp"])
    return jax.shard_map(body, mesh=mesh, in_specs=in_specs, out_specs=out_specs, check_vma=False)
```

```python
import functools

import jax
import jax.numpy as jnp
from jax import lax
from jax.experimental import pallas as pl
from jax.experimental.pallas import tpu as pltpu
from jax.sharding import PartitionSpec as P

MESH = pl.DeviceIdType.MESH
NT = (((1,), (1,)), ((), ()))
NN = (((1,), (0,)), ((), ()))
GRAD_SHARES = (1, 1)
SHARES = (4, 6, 6, 6, 4, 2)
GROUP = 4
FOLDS = 2
CORES = 2
LANES = 128
ROWS = 16


def kernel(
    n,
    lens_hbm,
    acts_hbm,
    grads_hbm,
    win_hbm,
    wout_hbm,
    q_hbm,
    res,
    lens,
    acts,
    grads,
    win,
    wout,
    q_own,
    qs,
    g_own,
    eg,
    stage,
    wide,
    gt,
    q_sem,
    grads_sem,
    acts_sem,
    send_sem,
    q_recv,
    eg_recv,
    res_recv,
):
    me = lax.axis_index("dp")
    n_groups = n // GROUP
    group, lane = me // GROUP, lax.rem(me, GROUP)
    core = lax.rem(me, CORES)
    pair = lane - core
    far_pair = CORES - pair
    tokens, ff = acts.shape
    rank, d = wout.shape
    ex = stage.shape[1]
    slots = ROWS // ex
    nq, part = qs.shape[1:]
    span = part // slots
    tiles = span // LANES
    half = tiles * ROWS
    cols = GROUP * nq
    units = CORES * n_groups

    backward = (group < n_groups - group).astype(jnp.int32)

    def peer_group(t):
        return lax.rem(group + t + backward * (n_groups - 2 * t), n_groups)

    def device(g, c):
        return g * GROUP + pair + c

    buddy = device(group, 1 - core)
    across = [group * GROUP + far_pair + c for c in range(CORES)]

    def start(source, target, sem):
        load = pltpu.make_async_copy(source, target, sem)
        load.start()
        return load

    def cuts(size, shares):
        edges = [size * sum(shares[:p]) // sum(shares) for p in range(len(shares) + 1)]
        return list(zip(edges[:-1], edges[1:]))

    def fetch(rows_hbm, rows, weights_hbm, weights, sem, cut):
        side = pl.ds(cut[0], cut[1] - cut[0])
        return (
            start(weights_hbm.at[:, side], weights.at[:, side], sem),
            start(rows_hbm.at[:, side], rows.at[:, side], sem),
        )

    def project(sums, rows, weights, cut):
        for h in range(2):
            side = slice(h * tokens // 2, (h + 1) * tokens // 2)
            term = lax.dot_general(
                rows[side, cut[0] : cut[1]],
                weights[:, cut[0] : cut[1]],
                NT,
                preferred_element_type=jnp.float32,
            )
            sums[h] = term if sums[h] is None else sums[h] + term

    def remote(source, target, recv_sem, other):
        return pltpu.make_async_remote_copy(
            src_ref=source,
            dst_ref=target,
            send_sem=send_sem,
            recv_sem=recv_sem,
            device_id={"dp": other},
            device_id_type=MESH,
        )

    def send(source, target, recv_sem, other):
        copy = remote(source, target, recv_sem, other)
        copy.start()
        return copy

    mine = pl.ds(pl.multiple_of(core * part, LANES), part)
    barrier = pltpu.get_barrier_semaphore()
    column = [device(peer_group(t), c) for t in range(1, n_groups) for c in range(CORES)]
    partners = across + [buddy] + column
    waiting = list(partners)

    def announce(count):
        for other in waiting[:count]:
            pl.semaphore_signal(barrier, inc=1, device_id={"dp": other}, device_id_type=MESH)
        del waiting[:count]

    grad_cuts, cut = cuts(d, GRAD_SHARES), cuts(ff, SHARES)
    load_q = start(q_hbm, q_own, q_sem)
    announce(3)
    load_lens = start(lens_hbm, lens, grads_sem.at[0])
    load_grads, load_acts = [], []
    for p in range(len(grad_cuts)):
        load_grads.append(fetch(grads_hbm, grads, wout_hbm, wout, grads_sem.at[p], grad_cuts[p]))
        announce(1)
    for p in range(len(cut)):
        load_acts.append(fetch(acts_hbm, acts, win_hbm, win, acts_sem.at[p], cut[p]))
        announce(1)
    announce(len(waiting))

    load_q.wait()
    fold = part // FOLDS
    copies = []
    for c, other in ((0, across[0]), (1, across[1]), (1 - core, buddy)):
        for f in range(FOLDS):
            side = pl.ds(pl.multiple_of(c * part + f * fold, LANES), fold)
            into = qs.at[lane, :, pl.ds(f * fold, fold)]
            copies.append(remote(q_own.at[:, side], into, q_recv.at[f], other))
    queries_sent = list(copies)

    def meet():
        pl.semaphore_wait(barrier, len(partners))
        for copy in queries_sent:
            copy.start()

    lower_half = group < n_groups // 2
    load_mine = start(q_hbm.at[:, mine], qs.at[lane], q_sem)

    at_row = lax.broadcasted_iota(jnp.int32, (8, tokens), 0)
    per_block = 8 // ex

    def masks():
        token = lax.broadcasted_iota(jnp.int32, (8, tokens), 1)
        row_ex = lax.rem(at_row, ex)
        begin = jnp.int32(0)
        mask = jnp.zeros((8, tokens), jnp.float32)
        for e in range(ex):
            end = begin + lens[0, e]
            mask = jnp.where((row_ex == e) & (token >= begin) & (token < end), 1.0, mask)
            begin = end
        return mask

    def widen(odd, mask):
        for c, t in [(c, t) for c in range(CORES) for t in range(tiles)]:
            blocks = []
            for b in range(ROWS // 8):
                block = None
                for j in range(per_block):
                    s = b * per_block + j
                    row = 2 * ((c * slots + s) * tiles + t) + odd
                    one = jnp.broadcast_to(gt[row : row + 1], (8, tokens))
                    block = one if block is None else jnp.where(at_row >= j * ex, one, block)
                blocks.append(block * mask)
            at = c * half + t * ROWS
            wide[odd, at : at + ROWS] = jnp.concatenate(blocks, axis=0).astype(jnp.bfloat16)

    def produce(meet_late):
        if not meet_late:
            meet()
        load_lens.wait()
        of_grads = [None, None]
        for p in range(len(grad_cuts)):
            for load in load_grads[p]:
                load.wait()
            project(of_grads, grads, wout, grad_cuts[p])

        def keep():
            gt[...] = jnp.concatenate(of_grads, axis=0).T

        if meet_late:
            keep()
            pl.when(me >= CORES)(meet)
        of_acts = [None, None]
        for p in range(len(cut)):
            for load in load_acts[p]:
                load.wait()
            project(of_acts, acts, win, cut[p])
            if p == 0 and not meet_late:
                keep()
            if p == 1:
                mask = masks()
                widen(0, mask)
            if p == 2:
                widen(1, mask)
        proj_acts = jnp.concatenate(of_acts, axis=0).astype(jnp.bfloat16)
        twice = jnp.concatenate([proj_acts, proj_acts], axis=1)
        even = lax.dot_general(wide[0], twice, NN, preferred_element_type=jnp.float32)
        odd = lax.dot_general(wide[1], twice, NN, preferred_element_type=jnp.float32)
        lower = lax.broadcasted_iota(jnp.int32, (CORES * half, 2 * rank), 1) < rank
        both = jnp.where(lower, even, odd).astype(jnp.bfloat16)
        for c in range(CORES):
            g_own[c] = both[c * half : (c + 1) * half]

    pl.when(lower_half)(lambda: produce(True))
    pl.when(jnp.logical_not(lower_half))(lambda: produce(False))

    pl.when(me < CORES)(meet)
    unit = group * CORES + core
    home = group == 0
    away = jnp.logical_not(home)
    kind = jnp.where(home, 0, 1)
    for c in range(CORES):
        for t in range(1, n_groups):
            copies.append(send(g_own.at[c], eg.at[unit], eg_recv.at[kind], device(peer_group(t), c)))
    copies.append(send(g_own.at[1 - core], eg.at[unit], eg_recv.at[kind], buddy))
    eg[unit] = g_own[core]

    load_mine.wait()

    def queries_here(f):
        others = qs.at[pl.ds(0, GROUP - 1), :, pl.ds(f * fold, fold)]
        pltpu.make_async_copy(others, others, q_recv.at[f]).wait()

    slot = core * n_groups + group

    def arrived(count, sem):
        block = eg.at[pl.ds(0, count)]
        pltpu.make_async_copy(block, block, sem).wait()

    def score(low, high, ready=lambda f: None):
        stacked = []
        for u in range(low, high):
            one = eg[u]
            stacked.append(
                jnp.concatenate([one[ROWS * t : ROWS * (t + 1)] for t in range(tiles)], axis=1)
            )
        stacked = jnp.concatenate(stacked, axis=0)
        scores = [None] * (high - low)
        for s in range(slots):
            if s % (slots // FOLDS) == 0:
                ready(s // (slots // FOLDS))
            queries = qs[:, :, s * span : (s + 1) * span].reshape(cols, span)
            term = lax.dot_general(stacked, queries, NT, preferred_element_type=jnp.float32)
            for u in range(high - low):
                row = ROWS * u + ex * s
                piece = term[row : row + ex]
                scores[u] = piece if scores[u] is None else scores[u] + piece
        for u in range(low, high):
            stage[u] = scores[u - low]

    def deliver(u, other):
        return remote(stage.at[u], res.at[slot], res_recv, other)

    to_buddy = deliver(group * CORES + 1 - core, buddy)
    to_home = [deliver(c, device(0, c)) for c in range(CORES)]
    onward = []
    for t in range(1, n_groups):
        g = peer_group(t)
        for c in range(CORES):
            onward.append((g > 0, deliver(g * CORES + c, device(g, c))))

    def settle():
        to_buddy.start()
        res[slot] = stage[unit]

    pl.when(home)(lambda: arrived(1, eg_recv.at[0]))
    pl.when(away)(lambda: arrived(CORES, eg_recv.at[0]))
    score(0, CORES, queries_here)
    pl.when(home)(settle)

    @pl.when(away)
    def _():
        for copy in to_home:
            copy.start()

    pl.when(home)(lambda: arrived(units - CORES, eg_recv.at[1]))
    pl.when(away)(lambda: arrived(units - CORES - 1, eg_recv.at[1]))
    score(CORES, units)
    for wanted, copy in onward:
        pl.when(wanted)(copy.start)
    pl.when(away)(settle)
    rest = res.at[pl.ds(0, units - 1)]
    pltpu.make_async_copy(rest, rest, res_recv).wait()
    for copy in copies + [to_buddy]:
        copy.wait_send()

    @pl.when(away)
    def _():
        for copy in to_home:
            copy.wait_send()

    for wanted, copy in onward:
        pl.when(wanted)(copy.wait_send)


def local(n, activations, out_grads, lengths, proj_in, proj_out, queries):
    tokens, ff = activations.shape
    d = out_grads.shape[1]
    rank = proj_in.shape[1]
    ex = lengths.shape[1]
    nq, params = queries.shape
    n_groups = n // GROUP
    units = CORES * n_groups
    rows = ex * params // LANES
    bf16, f32 = jnp.bfloat16, jnp.float32
    dma = pltpu.SemaphoreType.DMA
    hbm = pl.BlockSpec(memory_space=pltpu.MemorySpace.HBM)
    parts = pl.pallas_call(
        functools.partial(kernel, n),
        out_shape=jax.ShapeDtypeStruct((units, ex, GROUP * nq), f32),
        in_specs=[hbm] * 6,
        out_specs=pl.BlockSpec(memory_space=pltpu.MemorySpace.VMEM),
        scratch_shapes=[
            pltpu.SMEM((1, ex), jnp.int32),
            pltpu.VMEM((tokens, ff), bf16),
            pltpu.VMEM((tokens, d), bf16),
            pltpu.VMEM((rank, ff), bf16),
            pltpu.VMEM((rank, d), bf16),
            pltpu.VMEM((nq, params), bf16),
            pltpu.VMEM((GROUP, nq, params // CORES), bf16),
            pltpu.VMEM((CORES, rows // CORES, LANES), bf16),
            pltpu.VMEM((units, rows // CORES, LANES), bf16),
            pltpu.VMEM((units, ex, GROUP * nq), f32),
            pltpu.VMEM((2, rows, tokens), bf16),
            pltpu.VMEM((rank, tokens), f32),
            dma,
            dma((len(GRAD_SHARES),)),
            dma((len(SHARES),)),
            dma,
            dma((FOLDS,)),
            dma((2,)),
            dma,
        ],
        compiler_params=pltpu.CompilerParams(
            collective_id=0, has_side_effects=True, vmem_limit_bytes=56500000
        ),
    )(pltpu.with_memory_space_constraint(lengths, pltpu.HBM), activations, out_grads, proj_in.T, proj_out.T, queries)
    total = parts[:n_groups] + parts[n_groups:]
    return total.swapaxes(0, 1).reshape(ex, nq * n).astype(bf16)


def solution(mesh):
    in_specs = (
        P(("parts", "dp"), None),
        P(("parts", "dp"), None),
        P(("parts", "dp"), None),
        P(),
        P(),
        P(("parts", "dp"), None),
    )
    out_specs = P(("parts", "dp"), None)
    body = functools.partial(local, mesh.shape["dp"])
    return jax.shard_map(body, mesh=mesh, in_specs=in_specs, out_specs=out_specs, check_vma=False)
```

```python
import functools

import jax
import jax.numpy as jnp
from jax import lax
from jax.experimental import pallas as pl
from jax.experimental.pallas import tpu as pltpu
from jax.sharding import PartitionSpec as P

MESH = pl.DeviceIdType.MESH
NT = (((1,), (1,)), ((), ()))
NN = (((1,), (0,)), ((), ()))
GRAD_SHARES = (1, 1)
SHARES = (4, 8, 8, 6, 2)
GROUP = 4
FOLDS = 2
CORES = 2
LANES = 128
ROWS = 16


def kernel(
    n,
    lens_hbm,
    acts_hbm,
    grads_hbm,
    win_hbm,
    wout_hbm,
    q_hbm,
    res,
    lens,
    acts,
    grads,
    win,
    wout,
    q_own,
    qs,
    g_own,
    eg,
    stage,
    wide,
    gt,
    q_sem,
    grads_sem,
    acts_sem,
    send_sem,
    q_recv,
    eg_recv,
    res_recv,
):
    me = lax.axis_index("dp")
    n_groups = n // GROUP
    group, lane = me // GROUP, lax.rem(me, GROUP)
    core = lax.rem(me, CORES)
    pair = lane - core
    far_pair = CORES - pair
    tokens, ff = acts.shape
    rank, d = wout.shape
    ex = stage.shape[1]
    slots = ROWS // ex
    nq, part = qs.shape[1:]
    span = part // slots
    tiles = span // LANES
    half = tiles * ROWS
    cols = GROUP * nq
    units = CORES * n_groups

    backward = (group < n_groups - group).astype(jnp.int32)

    def peer_group(t):
        return lax.rem(group + t + backward * (n_groups - 2 * t), n_groups)

    def device(g, c):
        return g * GROUP + pair + c

    buddy = device(group, 1 - core)
    across = [group * GROUP + far_pair + c for c in range(CORES)]

    def start(source, target, sem):
        load = pltpu.make_async_copy(source, target, sem)
        load.start()
        return load

    def cuts(size, shares):
        edges = [size * sum(shares[:p]) // sum(shares) for p in range(len(shares) + 1)]
        return list(zip(edges[:-1], edges[1:]))

    def fetch(rows_hbm, rows, weights_hbm, weights, sem, cut):
        side = pl.ds(cut[0], cut[1] - cut[0])
        return (
            start(weights_hbm.at[:, side], weights.at[:, side], sem),
            start(rows_hbm.at[:, side], rows.at[:, side], sem),
        )

    def project(sums, rows, weights, cut):
        for h in range(2):
            side = slice(h * tokens // 2, (h + 1) * tokens // 2)
            term = lax.dot_general(
                rows[side, cut[0] : cut[1]],
                weights[:, cut[0] : cut[1]],
                NT,
                preferred_element_type=jnp.float32,
            )
            sums[h] = term if sums[h] is None else sums[h] + term

    def remote(source, target, recv_sem, other):
        return pltpu.make_async_remote_copy(
            src_ref=source,
            dst_ref=target,
            send_sem=send_sem,
            recv_sem=recv_sem,
            device_id={"dp": other},
            device_id_type=MESH,
        )

    def send(source, target, recv_sem, other):
        copy = remote(source, target, recv_sem, other)
        copy.start()
        return copy

    mine = pl.ds(pl.multiple_of(core * part, LANES), part)
    barrier = pltpu.get_barrier_semaphore()
    column = [device(peer_group(t), c) for t in range(1, n_groups) for c in range(CORES)]
    partners = across + [buddy] + column
    waiting = list(partners)

    def announce(count):
        for other in waiting[:count]:
            pl.semaphore_signal(barrier, inc=1, device_id={"dp": other}, device_id_type=MESH)
        del waiting[:count]

    grad_cuts, cut = cuts(d, GRAD_SHARES), cuts(ff, SHARES)
    load_q = start(q_hbm, q_own, q_sem)
    announce(3)
    load_lens = start(lens_hbm, lens, grads_sem.at[0])
    load_grads, load_acts = [], []
    for p in range(len(grad_cuts)):
        load_grads.append(fetch(grads_hbm, grads, wout_hbm, wout, grads_sem.at[p], grad_cuts[p]))
        announce(1)
    for p in range(len(cut)):
        load_acts.append(fetch(acts_hbm, acts, win_hbm, win, acts_sem.at[p], cut[p]))
        announce(1)
    announce(len(waiting))

    load_q.wait()
    fold = part // FOLDS
    copies = []
    for c, other in ((0, across[0]), (1, across[1]), (1 - core, buddy)):
        for f in range(FOLDS):
            side = pl.ds(pl.multiple_of(c * part + f * fold, LANES), fold)
            into = qs.at[lane, :, pl.ds(f * fold, fold)]
            copies.append(remote(q_own.at[:, side], into, q_recv.at[f], other))
    queries_sent = list(copies)

    def meet():
        pl.semaphore_wait(barrier, len(partners))
        for copy in queries_sent:
            copy.start()

    lower_half = group < n_groups // 2

    at_row = lax.broadcasted_iota(jnp.int32, (8, tokens), 0)
    per_block = 8 // ex

    def masks():
        token = lax.broadcasted_iota(jnp.int32, (8, tokens), 1)
        row_ex = lax.rem(at_row, ex)
        begin = jnp.int32(0)
        mask = jnp.zeros((8, tokens), jnp.float32)
        for e in range(ex):
            end = begin + lens[0, e]
            mask = jnp.where((row_ex == e) & (token >= begin) & (token < end), 1.0, mask)
            begin = end
        return mask

    def widen(odd, mask):
        for c, t in [(c, t) for c in range(CORES) for t in range(tiles)]:
            blocks = []
            for b in range(ROWS // 8):
                block = None
                for j in range(per_block):
                    s = b * per_block + j
                    row = 2 * ((c * slots + s) * tiles + t) + odd
                    one = jnp.broadcast_to(gt[row : row + 1], (8, tokens))
                    block = one if block is None else jnp.where(at_row >= j * ex, one, block)
                blocks.append(block * mask)
            at = c * half + t * ROWS
            wide[odd, at : at + ROWS] = jnp.concatenate(blocks, axis=0).astype(jnp.bfloat16)

    def produce(meet_late):
        if not meet_late:
            meet()
        load_lens.wait()
        of_grads = [None, None]
        for p in range(len(grad_cuts)):
            for load in load_grads[p]:
                load.wait()
            project(of_grads, grads, wout, grad_cuts[p])

        def keep():
            gt[...] = jnp.concatenate(of_grads, axis=0).T

        if meet_late:
            keep()
            pl.when(me >= CORES)(meet)
        of_acts = [None, None]
        for p in range(len(cut)):
            for load in load_acts[p]:
                load.wait()
            project(of_acts, acts, win, cut[p])
            if p == 0 and not meet_late:
                keep()
            if p == 1:
                mask = masks()
                widen(0, mask)
            if p == 2:
                widen(1, mask)
        proj_acts = jnp.concatenate(of_acts, axis=0).astype(jnp.bfloat16)
        twice = jnp.concatenate([proj_acts, proj_acts], axis=1)
        even = lax.dot_general(wide[0], twice, NN, preferred_element_type=jnp.float32)
        odd = lax.dot_general(wide[1], twice, NN, preferred_element_type=jnp.float32)
        lower = lax.broadcasted_iota(jnp.int32, (CORES * half, 2 * rank), 1) < rank
        both = jnp.where(lower, even, odd).astype(jnp.bfloat16)
        for c in range(CORES):
            g_own[c] = both[c * half : (c + 1) * half]

    pl.when(lower_half)(lambda: produce(True))
    pl.when(jnp.logical_not(lower_half))(lambda: produce(False))

    pl.when(me < CORES)(meet)
    unit = group * CORES + core
    home = group == 0
    away = jnp.logical_not(home)
    kind = jnp.where(home, 0, 1)
    for c in range(CORES):
        for t in range(1, n_groups):
            copies.append(send(g_own.at[c], eg.at[unit], eg_recv.at[kind], device(peer_group(t), c)))
    copies.append(send(g_own.at[1 - core], eg.at[unit], eg_recv.at[kind], buddy))
    eg[unit] = g_own[core]

    qs[lane] = q_own[:, mine]

    def queries_here(f):
        others = qs.at[pl.ds(0, GROUP - 1), :, pl.ds(f * fold, fold)]
        pltpu.make_async_copy(others, others, q_recv.at[f]).wait()

    slot = core * n_groups + group

    def arrived(count, sem):
        block = eg.at[pl.ds(0, count)]
        pltpu.make_async_copy(block, block, sem).wait()

    def score(low, high, ready=lambda f: None):
        stacked = []
        for u in range(low, high):
            one = eg[u]
            stacked.append(
                jnp.concatenate([one[ROWS * t : ROWS * (t + 1)] for t in range(tiles)], axis=1)
            )
        stacked = jnp.concatenate(stacked, axis=0)
        scores = [None] * (high - low)
        for s in range(slots):
            if s % (slots // FOLDS) == 0:
                ready(s // (slots // FOLDS))
            queries = qs[:, :, s * span : (s + 1) * span].reshape(cols, span)
            term = lax.dot_general(stacked, queries, NT, preferred_element_type=jnp.float32)
            for u in range(high - low):
                row = ROWS * u + ex * s
                piece = term[row : row + ex]
                scores[u] = piece if scores[u] is None else scores[u] + piece
        for u in range(low, high):
            stage[u] = scores[u - low]

    def deliver(u, other):
        return remote(stage.at[u], res.at[slot], res_recv, other)

    to_buddy = deliver(group * CORES + 1 - core, buddy)
    to_home = [deliver(c, device(0, c)) for c in range(CORES)]
    onward = []
    for t in range(1, n_groups):
        g = peer_group(t)
        for c in range(CORES):
            onward.append((g > 0, deliver(g * CORES + c, device(g, c))))

    def settle():
        to_buddy.start()
        res[slot] = stage[unit]

    pl.when(home)(lambda: arrived(1, eg_recv.at[0]))
    pl.when(away)(lambda: arrived(CORES, eg_recv.at[0]))
    score(0, CORES, queries_here)
    pl.when(home)(settle)

    @pl.when(away)
    def _():
        for copy in to_home:
            copy.start()

    pl.when(home)(lambda: arrived(units - CORES, eg_recv.at[1]))
    pl.when(away)(lambda: arrived(units - CORES - 1, eg_recv.at[1]))
    score(CORES, units)
    for wanted, copy in onward:
        pl.when(wanted)(copy.start)
    pl.when(away)(settle)
    rest = res.at[pl.ds(0, units - 1)]
    pltpu.make_async_copy(rest, rest, res_recv).wait()
    for copy in copies + [to_buddy]:
        copy.wait_send()

    @pl.when(away)
    def _():
        for copy in to_home:
            copy.wait_send()

    for wanted, copy in onward:
        pl.when(wanted)(copy.wait_send)


def local(n, activations, out_grads, lengths, proj_in, proj_out, queries):
    tokens, ff = activations.shape
    d = out_grads.shape[1]
    rank = proj_in.shape[1]
    ex = lengths.shape[1]
    nq, params = queries.shape
    n_groups = n // GROUP
    units = CORES * n_groups
    rows = ex * params // LANES
    bf16, f32 = jnp.bfloat16, jnp.float32
    dma = pltpu.SemaphoreType.DMA
    hbm = pl.BlockSpec(memory_space=pltpu.MemorySpace.HBM)
    parts = pl.pallas_call(
        functools.partial(kernel, n),
        out_shape=jax.ShapeDtypeStruct((units, ex, GROUP * nq), f32),
        in_specs=[hbm] * 6,
        out_specs=pl.BlockSpec(memory_space=pltpu.MemorySpace.VMEM),
        scratch_shapes=[
            pltpu.SMEM((1, ex), jnp.int32),
            pltpu.VMEM((tokens, ff), bf16),
            pltpu.VMEM((tokens, d), bf16),
            pltpu.VMEM((rank, ff), bf16),
            pltpu.VMEM((rank, d), bf16),
            pltpu.VMEM((nq, params), bf16),
            pltpu.VMEM((GROUP, nq, params // CORES), bf16),
            pltpu.VMEM((CORES, rows // CORES, LANES), bf16),
            pltpu.VMEM((units, rows // CORES, LANES), bf16),
            pltpu.VMEM((units, ex, GROUP * nq), f32),
            pltpu.VMEM((2, rows, tokens), bf16),
            pltpu.VMEM((rank, tokens), f32),
            dma,
            dma((len(GRAD_SHARES),)),
            dma((len(SHARES),)),
            dma,
            dma((FOLDS,)),
            dma((2,)),
            dma,
        ],
        compiler_params=pltpu.CompilerParams(
            collective_id=0, has_side_effects=True, vmem_limit_bytes=56500000
        ),
    )(pltpu.with_memory_space_constraint(lengths, pltpu.HBM), activations, out_grads, proj_in.T, proj_out.T, queries)
    total = parts[:n_groups] + parts[n_groups:]
    return total.swapaxes(0, 1).reshape(ex, nq * n).astype(bf16)


def solution(mesh):
    in_specs = (
        P(("parts", "dp"), None),
        P(("parts", "dp"), None),
        P(("parts", "dp"), None),
        P(),
        P(),
        P(("parts", "dp"), None),
    )
    out_specs = P(("parts", "dp"), None)
    body = functools.partial(local, mesh.shape["dp"])
    return jax.shard_map(body, mesh=mesh, in_specs=in_specs, out_specs=out_specs, check_vma=False)
```

```python
import functools

import jax
import jax.numpy as jnp
from jax import lax
from jax.experimental import pallas as pl
from jax.experimental.pallas import tpu as pltpu
from jax.sharding import PartitionSpec as P

MESH = pl.DeviceIdType.MESH
NT = (((1,), (1,)), ((), ()))
NN = (((1,), (0,)), ((), ()))
GRAD_SHARES = (1, 1)
SHARES = (4, 8, 8, 6, 2)
GROUP = 4
FOLDS = 4
CORES = 2
LANES = 128
ROWS = 16


def kernel(
    n,
    lens_hbm,
    acts_hbm,
    grads_hbm,
    win_hbm,
    wout_hbm,
    q_hbm,
    res,
    lens,
    acts,
    grads,
    win,
    wout,
    q_own,
    qs,
    g_own,
    eg,
    stage,
    wide,
    gt,
    q_sem,
    grads_sem,
    acts_sem,
    send_sem,
    q_recv,
    eg_recv,
    res_recv,
):
    me = lax.axis_index("dp")
    n_groups = n // GROUP
    group, lane = me // GROUP, lax.rem(me, GROUP)
    core = lax.rem(me, CORES)
    pair = lane - core
    far_pair = CORES - pair
    tokens, ff = acts.shape
    rank, d = wout.shape
    ex = stage.shape[1]
    slots = ROWS // ex
    nq, part = qs.shape[1:]
    span = part // slots
    tiles = span // LANES
    half = tiles * ROWS
    cols = GROUP * nq
    units = CORES * n_groups

    backward = (group < n_groups - group).astype(jnp.int32)

    def peer_group(t):
        return lax.rem(group + t + backward * (n_groups - 2 * t), n_groups)

    def device(g, c):
        return g * GROUP + pair + c

    buddy = device(group, 1 - core)
    across = [group * GROUP + far_pair + c for c in range(CORES)]

    def start(source, target, sem):
        load = pltpu.make_async_copy(source, target, sem)
        load.start()
        return load

    def cuts(size, shares):
        edges = [size * sum(shares[:p]) // sum(shares) for p in range(len(shares) + 1)]
        return list(zip(edges[:-1], edges[1:]))

    def fetch(rows_hbm, rows, weights_hbm, weights, sem, cut):
        side = pl.ds(cut[0], cut[1] - cut[0])
        return (
            start(weights_hbm.at[:, side], weights.at[:, side], sem),
            start(rows_hbm.at[:, side], rows.at[:, side], sem),
        )

    def project(sums, rows, weights, cut):
        for h in range(2):
            side = slice(h * tokens // 2, (h + 1) * tokens // 2)
            term = lax.dot_general(
                rows[side, cut[0] : cut[1]],
                weights[:, cut[0] : cut[1]],
                NT,
                preferred_element_type=jnp.float32,
            )
            sums[h] = term if sums[h] is None else sums[h] + term

    def remote(source, target, recv_sem, other):
        return pltpu.make_async_remote_copy(
            src_ref=source,
            dst_ref=target,
            send_sem=send_sem,
            recv_sem=recv_sem,
            device_id={"dp": other},
            device_id_type=MESH,
        )

    def send(source, target, recv_sem, other):
        copy = remote(source, target, recv_sem, other)
        copy.start()
        return copy

    mine = pl.ds(pl.multiple_of(core * part, LANES), part)
    barrier = pltpu.get_barrier_semaphore()
    column = [device(peer_group(t), c) for t in range(1, n_groups) for c in range(CORES)]
    partners = across + [buddy] + column
    waiting = list(partners)

    def announce(count):
        for other in waiting[:count]:
            pl.semaphore_signal(barrier, inc=1, device_id={"dp": other}, device_id_type=MESH)
        del waiting[:count]

    grad_cuts, cut = cuts(d, GRAD_SHARES), cuts(ff, SHARES)
    load_q = start(q_hbm, q_own, q_sem)
    announce(3)
    load_lens = start(lens_hbm, lens, grads_sem.at[0])
    load_grads, load_acts = [], []
    for p in range(len(grad_cuts)):
        load_grads.append(fetch(grads_hbm, grads, wout_hbm, wout, grads_sem.at[p], grad_cuts[p]))
        announce(1)
    for p in range(len(cut)):
        load_acts.append(fetch(acts_hbm, acts, win_hbm, win, acts_sem.at[p], cut[p]))
        announce(1)
    announce(len(waiting))

    load_q.wait()
    fold = part // FOLDS
    copies = []
    for c, other in ((0, across[0]), (1, across[1]), (1 - core, buddy)):
        for f in range(FOLDS):
            side = pl.ds(pl.multiple_of(c * part + f * fold, LANES), fold)
            into = qs.at[lane, :, pl.ds(f * fold, fold)]
            copies.append(remote(q_own.at[:, side], into, q_recv.at[f], other))
    queries_sent = list(copies)

    def meet():
        pl.semaphore_wait(barrier, len(partners))
        for copy in queries_sent:
            copy.start()

    lower_half = group < n_groups // 2

    at_row = lax.broadcasted_iota(jnp.int32, (8, tokens), 0)
    per_block = 8 // ex

    def masks():
        token = lax.broadcasted_iota(jnp.int32, (8, tokens), 1)
        row_ex = lax.rem(at_row, ex)
        begin = jnp.int32(0)
        mask = jnp.zeros((8, tokens), jnp.float32)
        for e in range(ex):
            end = begin + lens[0, e]
            mask = jnp.where((row_ex == e) & (token >= begin) & (token < end), 1.0, mask)
            begin = end
        return mask

    def widen(odd, mask):
        for c, t in [(c, t) for c in range(CORES) for t in range(tiles)]:
            blocks = []
            for b in range(ROWS // 8):
                block = None
                for j in range(per_block):
                    s = b * per_block + j
                    row = 2 * ((c * slots + s) * tiles + t) + odd
                    one = jnp.broadcast_to(gt[row : row + 1], (8, tokens))
                    block = one if block is None else jnp.where(at_row >= j * ex, one, block)
                blocks.append(block * mask)
            at = c * half + t * ROWS
            wide[odd, at : at + ROWS] = jnp.concatenate(blocks, axis=0).astype(jnp.bfloat16)

    def produce(meet_late):
        if not meet_late:
            meet()
        load_lens.wait()
        of_grads = [None, None]
        for p in range(len(grad_cuts)):
            for load in load_grads[p]:
                load.wait()
            project(of_grads, grads, wout, grad_cuts[p])

        def keep():
            gt[...] = jnp.concatenate(of_grads, axis=0).T

        if meet_late:
            keep()
            pl.when(me >= CORES)(meet)
        of_acts = [None, None]
        for p in range(len(cut)):
            for load in load_acts[p]:
                load.wait()
            project(of_acts, acts, win, cut[p])
            if p == 0 and not meet_late:
                keep()
            if p == 1:
                mask = masks()
                widen(0, mask)
            if p == 2:
                widen(1, mask)
        proj_acts = jnp.concatenate(of_acts, axis=0).astype(jnp.bfloat16)
        twice = jnp.concatenate([proj_acts, proj_acts], axis=1)
        even = lax.dot_general(wide[0], twice, NN, preferred_element_type=jnp.float32)
        odd = lax.dot_general(wide[1], twice, NN, preferred_element_type=jnp.float32)
        lower = lax.broadcasted_iota(jnp.int32, (CORES * half, 2 * rank), 1) < rank
        both = jnp.where(lower, even, odd).astype(jnp.bfloat16)
        for c in range(CORES):
            g_own[c] = both[c * half : (c + 1) * half]

    pl.when(lower_half)(lambda: produce(True))
    pl.when(jnp.logical_not(lower_half))(lambda: produce(False))

    pl.when(me < CORES)(meet)
    unit = group * CORES + core
    home = group == 0
    away = jnp.logical_not(home)
    kind = jnp.where(home, 0, 1)
    for c in range(CORES):
        for t in range(1, n_groups):
            copies.append(send(g_own.at[c], eg.at[unit], eg_recv.at[kind], device(peer_group(t), c)))
    copies.append(send(g_own.at[1 - core], eg.at[unit], eg_recv.at[kind], buddy))
    eg[unit] = g_own[core]

    qs[lane] = q_own[:, mine]

    def queries_here(f):
        others = qs.at[pl.ds(0, GROUP - 1), :, pl.ds(f * fold, fold)]
        pltpu.make_async_copy(others, others, q_recv.at[f]).wait()

    slot = core * n_groups + group

    def arrived(count, sem):
        block = eg.at[pl.ds(0, count)]
        pltpu.make_async_copy(block, block, sem).wait()

    def score(low, high, ready=lambda f: None):
        stacked = []
        for u in range(low, high):
            one = eg[u]
            stacked.append(
                jnp.concatenate([one[ROWS * t : ROWS * (t + 1)] for t in range(tiles)], axis=1)
            )
        stacked = jnp.concatenate(stacked, axis=0)
        scores = [None] * (high - low)
        for s in range(slots):
            if s % (slots // FOLDS) == 0:
                ready(s // (slots // FOLDS))
            queries = qs[:, :, s * span : (s + 1) * span].reshape(cols, span)
            term = lax.dot_general(stacked, queries, NT, preferred_element_type=jnp.float32)
            for u in range(high - low):
                row = ROWS * u + ex * s
                piece = term[row : row + ex]
                scores[u] = piece if scores[u] is None else scores[u] + piece
        for u in range(low, high):
            stage[u] = scores[u - low]

    def deliver(u, other):
        return remote(stage.at[u], res.at[slot], res_recv, other)

    to_buddy = deliver(group * CORES + 1 - core, buddy)
    to_home = [deliver(c, device(0, c)) for c in range(CORES)]
    onward = []
    for t in range(1, n_groups):
        g = peer_group(t)
        for c in range(CORES):
            onward.append((g > 0, deliver(g * CORES + c, device(g, c))))

    def settle():
        to_buddy.start()
        res[slot] = stage[unit]

    pl.when(home)(lambda: arrived(1, eg_recv.at[0]))
    pl.when(away)(lambda: arrived(CORES, eg_recv.at[0]))
    score(0, CORES, queries_here)
    pl.when(home)(settle)

    @pl.when(away)
    def _():
        for copy in to_home:
            copy.start()

    pl.when(home)(lambda: arrived(units - CORES, eg_recv.at[1]))
    pl.when(away)(lambda: arrived(units - CORES - 1, eg_recv.at[1]))
    score(CORES, units)
    for wanted, copy in onward:
        pl.when(wanted)(copy.start)
    pl.when(away)(settle)
    rest = res.at[pl.ds(0, units - 1)]
    pltpu.make_async_copy(rest, rest, res_recv).wait()
    for copy in copies + [to_buddy]:
        copy.wait_send()

    @pl.when(away)
    def _():
        for copy in to_home:
            copy.wait_send()

    for wanted, copy in onward:
        pl.when(wanted)(copy.wait_send)


def local(n, activations, out_grads, lengths, proj_in, proj_out, queries):
    tokens, ff = activations.shape
    d = out_grads.shape[1]
    rank = proj_in.shape[1]
    ex = lengths.shape[1]
    nq, params = queries.shape
    n_groups = n // GROUP
    units = CORES * n_groups
    rows = ex * params // LANES
    bf16, f32 = jnp.bfloat16, jnp.float32
    dma = pltpu.SemaphoreType.DMA
    hbm = pl.BlockSpec(memory_space=pltpu.MemorySpace.HBM)
    parts = pl.pallas_call(
        functools.partial(kernel, n),
        out_shape=jax.ShapeDtypeStruct((units, ex, GROUP * nq), f32),
        in_specs=[hbm] * 6,
        out_specs=pl.BlockSpec(memory_space=pltpu.MemorySpace.VMEM),
        scratch_shapes=[
            pltpu.SMEM((1, ex), jnp.int32),
            pltpu.VMEM((tokens, ff), bf16),
            pltpu.VMEM((tokens, d), bf16),
            pltpu.VMEM((rank, ff), bf16),
            pltpu.VMEM((rank, d), bf16),
            pltpu.VMEM((nq, params), bf16),
            pltpu.VMEM((GROUP, nq, params // CORES), bf16),
            pltpu.VMEM((CORES, rows // CORES, LANES), bf16),
            pltpu.VMEM((units, rows // CORES, LANES), bf16),
            pltpu.VMEM((units, ex, GROUP * nq), f32),
            pltpu.VMEM((2, rows, tokens), bf16),
            pltpu.VMEM((rank, tokens), f32),
            dma,
            dma((len(GRAD_SHARES),)),
            dma((len(SHARES),)),
            dma,
            dma((FOLDS,)),
            dma((2,)),
            dma,
        ],
        compiler_params=pltpu.CompilerParams(
            collective_id=0, has_side_effects=True, vmem_limit_bytes=56500000
        ),
    )(pltpu.with_memory_space_constraint(lengths, pltpu.HBM), activations, out_grads, proj_in.T, proj_out.T, queries)
    total = parts[:n_groups] + parts[n_groups:]
    return total.swapaxes(0, 1).reshape(ex, nq * n).astype(bf16)


def solution(mesh):
    in_specs = (
        P(("parts", "dp"), None),
        P(("parts", "dp"), None),
        P(("parts", "dp"), None),
        P(),
        P(),
        P(("parts", "dp"), None),
    )
    out_specs = P(("parts", "dp"), None)
    body = functools.partial(local, mesh.shape["dp"])
    return jax.shard_map(body, mesh=mesh, in_specs=in_specs, out_specs=out_specs, check_vma=False)
```
